512 devices in a mesh: mem: 8 (over y, core), space: 64 (over x, z).
Axes of the slice: x: 4, y: 4, z: 16, core: 2. Of those that a mesh axis runs over, the one named last changes fastest.
Arguments:
- members: float32 [64, 1024, 1024], P('mem', 'space'), may hold values from -6 to 6
- flow_east: float32 [1024, 1024], P('space'), may hold values from -0.2 to 0.2
- flow_north: float32 [1024, 1024], P('space'), may hold values from -0.2 to 0.2
- mixing: float32 [1024, 1024], P('space'), may hold values from 0.05 to 0.24
- land_mask: int32 [1024, 1024], P('space'), may hold values 0 or 1
- sensor_cell: int32 [131072], P('space'), may hold values from 0 to 16383, as said below
- sensor_value: float32 [131072], P('space'), may hold values from -6 to 6
- sensor_noise: float32 [131072], P('space'), may hold values from 0.25 to 4
- tile_lists: int32 [1024, 8, 256], P('space', 'mem'), may hold values from 0 to 6143, as said below
- tile_counts: int32 [1024, 8], P('space', 'mem'), may hold values from 0 to 256, as said below
Outputs:
- analysis: float32 [64, 1024, 1024], P(None, 'space', 'mem')
The draws below stay inside these ranges and needn't reach their ends.
Inputs may be any that keep to these rules, and one draw needn't show every extreme that they name: Sensor j belongs to strip j // 2048: sensor_cell[j] // 1024 is its row within the strip's 16 rows and sensor_cell[j] % 1024 its column. `tile_lists`: for a tile in strip t an entry e names sensor (t - 1) * 2048 + e; the used entries of a tile are distinct sensors that exist, within 16 cells of the tile. `tile_counts`: at most 256, reached by some tile of every strip in every draw.
All inputs are finite; a program needn't handle non-finite values. No bound on the sum of `land_mask` on one device may be relied on, other than what follows from the above.
Results may differ from the reference program's by a relative error of at most 0.0003.
Values sent between devices are 32-bit elements; how exact they have to be, the bound alone decides.
A program may use at most 64 MiB of HBM per device.

```python
import math
import jax
import jax.numpy as jnp
from jax import lax

M = 64
TW = 128
CY = 16
OBS_DEV = 2048
LMAX = 256
STEPS = 4
NSITER = 8
NX = 1024
NY = 1024
NOBS = 131072
RLOC = 8


def sensor_layout(key):
    base = jax.random.fold_in(key, 7)
    strips = NY // CY
    keys = jax.random.split(base, 6)
    rows_any = jax.random.randint(keys[0], (strips, OBS_DEV), 0, CY)
    cols_any = jax.random.randint(keys[1], (strips, OBS_DEV), 0, NX)
    dense_block = jax.random.randint(keys[2], (strips, 1), 0, NX // TW)
    rows_dense = CY // 4 + jax.random.randint(keys[3], (strips, OBS_DEV), 0, CY // 2)
    cols_dense = dense_block * TW + TW // 4 + jax.random.randint(keys[4], (strips, OBS_DEV), 0, TW // 2)
    shuffled = jax.vmap(lambda piece: jax.random.permutation(piece, OBS_DEV))(jax.random.split(keys[5], strips))
    dense = shuffled < OBS_DEV // 2
    rows = jnp.where(dense, rows_dense, rows_any)
    columns = jnp.where(dense, cols_dense, cols_any)
    return (rows * NX + columns).astype(jnp.int32)


def tile_tables(key):
    cells = sensor_layout(key)
    strips = NY // CY
    blocks = NX // TW
    total = strips * OBS_DEV
    sensor_row = (jnp.arange(strips, dtype=jnp.int32)[:, None] * CY + cells // NX).reshape(-1)
    sensor_col = (cells % NX).reshape(-1)

    def per_strip(strip_index):
        glob = (strip_index - 1) * OBS_DEV + jnp.arange(3 * OBS_DEV, dtype=jnp.int32)
        exists = (glob >= 0) & (glob < total)
        safe = jnp.clip(glob, 0, total - 1)
        pool_row = sensor_row[safe]
        pool_col = sensor_col[safe]
        tile_row = strip_index * CY + jnp.arange(CY, dtype=jnp.int32)
        middle = 2 * jnp.arange(blocks, dtype=jnp.int32) * TW + TW - 1
        rise = 2 * (pool_row[None, None, :] - tile_row[:, None, None])
        across = jnp.abs(2 * pool_col[None, None, :] - middle[None, :, None])
        across = jnp.minimum(across, 2 * NX - across)
        beyond = jnp.maximum(across - (TW - 1), 0)
        keyed = rise * rise + beyond * beyond
        inside = exists[None, None, :] & (keyed <= 4 * CY * CY)
        scores = jnp.where(inside, keyed, 2 ** 30)
        ordered = jnp.argsort(scores, axis=-1, stable=True)[..., :LMAX]
        counted = jnp.minimum(jnp.sum(inside.astype(jnp.int32), axis=-1), LMAX)
        return (ordered.astype(jnp.int32), counted.astype(jnp.int32))
    listed, counted = lax.map(per_strip, jnp.arange(strips, dtype=jnp.int32))
    return (listed.reshape(NY, blocks, LMAX), counted.reshape(NY, blocks))


def draw_sensor_cell(key, part):
    return sensor_layout(key).reshape(-1)


def draw_tile_lists(key, part):
    return tile_tables(key)[0]


def draw_tile_counts(key, part):
    return tile_tables(key)[1]


def plant(entries, stream_key, smallest, top_value):
    index_at = [jax.random.randint(jax.random.fold_in(stream_key, axis), (), 0, length) for axis, length in enumerate(entries.shape)]
    widest = entries.shape.index(max(entries.shape))
    next_to = index_at[:widest] + [(index_at[widest] + 1) % entries.shape[widest]] + index_at[widest + 1:]
    return entries.at[tuple(index_at)].set(smallest).at[tuple(next_to)].set(top_value)


def block_levels(rng, dims, shards, least, high):
    loudness = 1.0
    for dim, parts in shards:
        draws = jax.random.uniform(jax.random.fold_in(jax.random.fold_in(rng, 6), dim), (parts,), jnp.float32, least / len(shards), high / len(shards))
        loudness = loudness * jnp.repeat(jnp.exp(draws), dims[dim] // parts).reshape((-1,) + (1,) * (len(dims) - 1 - dim))
    return loudness


def centred(rng, dims, deviation, bound, shards=(), held_as=jnp.bfloat16):
    level = block_levels(rng, dims, shards, -0.22, 0.18) if shards else 1.0
    values = jax.random.normal(rng, dims, jnp.float32) * deviation * level
    return jnp.minimum(jnp.maximum(values, -bound), bound).astype(held_as)


def setup_inputs(seed: int = 0) -> dict:
    arg_keys = jax.random.split(jax.random.key(seed), 11)
    return {
        "members": centred(arg_keys[0], (M, NY, NX), 1.0, 6.0, ((0, 8), (1, 64)), jnp.float32),
        "flow_east": jnp.clip(jax.random.uniform(arg_keys[1], (NY, NX), jnp.float32, -0.2, 0.2) * block_levels(arg_keys[1], (NY, NX), ((0, 64),), -0.4, 0.0), -0.2, 0.2),
        "flow_north": jnp.clip(jax.random.uniform(arg_keys[2], (NY, NX), jnp.float32, -0.2, 0.2) * block_levels(arg_keys[2], (NY, NX), ((0, 64),), -0.4, 0.0), -0.2, 0.2),
        "mixing": jnp.clip(jnp.exp(math.log(0.24) - 1.5686159 * jax.random.uniform(arg_keys[3], (NY, NX), jnp.float32) ** block_levels(arg_keys[3], (NY, NX), ((0, 64),), -0.2, 0.2)), 0.05, 0.24),
        "land_mask": plant((jax.random.randint(arg_keys[4], (NY, NX), 0, 4) < 3).astype(jnp.int32), jax.random.fold_in(arg_keys[4], 1), 0, 1),
        "sensor_cell": draw_sensor_cell(jax.random.fold_in(arg_keys[10], 71), 0),
        "sensor_value": centred(arg_keys[6], (NOBS,), 1.0, 6.0, ((0, 64),), jnp.float32),
        "sensor_noise": jnp.clip(jnp.exp(math.log(4.0) - 2.7725887 * jax.random.uniform(arg_keys[7], (NOBS,), jnp.float32) ** block_levels(arg_keys[7], (NOBS,), ((0, 64),), -0.2, 0.2)), 0.25, 4.0),
        "tile_lists": draw_tile_lists(jax.random.fold_in(arg_keys[10], 71), 0),
        "tile_counts": draw_tile_counts(jax.random.fold_in(arg_keys[10], 71), 0),
    }


highest = lax.Precision.HIGHEST

def gaspari(ratio):
    capped = jnp.maximum(ratio, 1.0)
    inner = (((-0.25 * ratio + 0.5) * ratio + 0.625) * ratio - 5.0 / 3.0) * ratio * ratio + 1.0
    outer = ((((ratio / 12.0 - 0.5) * ratio + 0.625) * ratio + 5.0 / 3.0) * ratio - 5.0) * ratio + 4.0 - 2.0 / (3.0 * capped)
    return jnp.where(ratio <= 1.0, inner, jnp.where(ratio <= 2.0, outer, 0.0))

def advance(padded, flow_east, flow_north, mixing, ocean):
    centre = padded[:, 1:-1, :]
    northern = padded[:, 2:, :]
    southern = padded[:, :-2, :]
    eastern = jnp.roll(centre, -1, axis=2)
    western = jnp.roll(centre, 1, axis=2)
    carried = 0.5 * flow_east * (eastern - western) + 0.5 * flow_north * (northern - southern)
    spread = eastern + western + northern + southern - 4.0 * centre
    return ocean * (centre - carried + mixing * spread)

def analyse(ensemble, values, variance, sensor_row, sensor_col, usable, tile_row, tile_mid, fields, width_total):
    count_members = ensemble.shape[0]
    prior_mean = lax.optimization_barrier(jnp.mean(ensemble, axis=0))
    spread = ensemble - prior_mean
    depart = values - prior_mean
    offset_rows = sensor_row - tile_row[:, None]
    offset_cols = jnp.abs(sensor_col - tile_mid[:, None])
    offset_cols = jnp.minimum(offset_cols, width_total - offset_cols)
    offset_cols = jnp.maximum(offset_cols - (TW - 1) / 2.0, 0.0)
    distance = jnp.sqrt(offset_cols * offset_cols + offset_rows * offset_rows)
    safe_variance = jnp.where(usable, variance, 1.0)
    weight = jnp.where(usable, gaspari(distance / RLOC) / safe_variance, 0.0)
    gram_matrix = jnp.einsum('knl,jnl->nkj', spread * weight, spread, precision=highest)
    identity = jnp.eye(count_members, dtype=jnp.float32)
    normed = identity + gram_matrix / (count_members - 1)
    frobenius = jnp.sqrt(lax.optimization_barrier(jnp.sum(normed * normed, axis=(1, 2))))
    iterate = normed / frobenius[:, None, None]
    inverse_root = jnp.broadcast_to(identity, normed.shape)
    for repeat in range(NSITER):
        factor = 1.5 * identity - 0.5 * jnp.matmul(inverse_root, iterate, precision=highest)
        iterate = jnp.matmul(iterate, factor, precision=highest)
        inverse_root = jnp.matmul(factor, inverse_root, precision=highest)
    transform = inverse_root / jnp.sqrt(frobenius)[:, None, None]
    forcing = jnp.einsum('knl,nl->nk', spread, weight * depart, precision=highest)
    halfway = jnp.einsum('nkj,nj->nk', transform, forcing, precision=highest)
    shift_mean = jnp.einsum('nkj,nj->nk', transform, halfway, precision=highest) / (count_members - 1)
    mixture = transform + shift_mean[:, :, None]
    field_mean = lax.optimization_barrier(jnp.mean(fields, axis=0))
    return field_mean + jnp.einsum('jnc,njk->knc', fields - field_mean, mixture, precision=highest)

def reference(members, flow_east, flow_north, mixing, land_mask, sensor_cell, sensor_value, sensor_noise, tile_lists, tile_counts):
    ocean = land_mask.astype(jnp.float32)
    fields = members * ocean
    for repeat in range(STEPS):
        padded = jnp.pad(fields, ((0, 0), (1, 1), (0, 0)))
        fields = advance(padded, flow_east, flow_north, mixing, ocean)
    strips = NY // CY
    blocks = NX // TW
    sensor_strip = jnp.arange(NOBS, dtype=jnp.int32) // OBS_DEV
    flat_cell = sensor_strip * (CY * NX) + sensor_cell
    ensemble_all = jnp.take(fields.reshape(M, NY * NX), flat_cell, axis=1)
    sensor_row = (sensor_strip * CY + sensor_cell // NX).astype(jnp.float32)
    sensor_col = (sensor_cell % NX).astype(jnp.float32)
    slot_index = jnp.arange(LMAX, dtype=jnp.int32)
    tile_index = jnp.arange(CY * blocks, dtype=jnp.int32)

    def per_strip(strip_index):
        start = (strip_index * CY).astype(jnp.int32)
        chosen_slots = lax.dynamic_slice_in_dim(tile_lists, start, CY, 0).reshape(CY * blocks, LMAX)
        counts = lax.dynamic_slice_in_dim(tile_counts, start, CY, 0).reshape(CY * blocks)
        chosen = jnp.clip((strip_index - 1) * OBS_DEV + chosen_slots, 0, NOBS - 1).astype(jnp.int32)
        usable = slot_index[None, :] < counts[:, None]
        ensemble = jnp.take(ensemble_all, chosen, axis=1)
        tile_row = (start + tile_index // blocks).astype(jnp.float32)
        tile_mid = (tile_index % blocks * TW).astype(jnp.float32) + (TW - 1) / 2.0
        local_fields = lax.dynamic_slice_in_dim(fields, start, CY, 1).reshape(M, CY * blocks, TW)
        result = analyse(ensemble, sensor_value[chosen], sensor_noise[chosen], sensor_row[chosen], sensor_col[chosen], usable, tile_row, tile_mid, local_fields, float(NX))
        return result.reshape(M, CY, NX)
    analysed = lax.map(per_strip, jnp.arange(strips, dtype=jnp.int32))
    return jnp.transpose(analysed, (1, 0, 2, 3)).reshape(M, NY, NX)
```

```python
import functools

import jax
import jax.numpy as jnp
from jax import lax
from jax.experimental import pallas as pl
from jax.experimental.pallas import tpu as pltpu
from jax.sharding import PartitionSpec as P

TW = 128
STEPS = 4
NSITER = 8
RLOC = 8
EDGE = 16
MESH = pl.DeviceIdType.MESH
VMEM = pltpu.VMEM
f32 = jnp.float32
bf16 = jnp.bfloat16
i32 = jnp.int32


def split(x):
    high = x.astype(bf16)
    return high, (x - high.astype(f32)).astype(bf16)


def dot_nt(a, b):
    return lax.dot_general(a, b, (((1,), (1,)), ((), ())), preferred_element_type=f32)


def dot_nn(a, b):
    return jnp.dot(a, b, preferred_element_type=f32)


def gaspari(ratio):
    capped = jnp.maximum(ratio, 1.0)
    inner = (((-0.25 * ratio + 0.5) * ratio + 0.625) * ratio - 5.0 / 3.0) * ratio * ratio + 1.0
    outer = (
        ((((ratio / 12.0 - 0.5) * ratio + 0.625) * ratio + 5.0 / 3.0) * ratio - 5.0) * ratio
        + 4.0
        - 2.0 / (3.0 * capped)
    )
    return jnp.where(ratio <= 1.0, inner, jnp.where(ratio <= 2.0, outer, 0.0))


def forecast_kernel(
    strips, groups,
    members, flow_east, flow_north, mixing, land, lists,
    window, lists_prev, lists_next,
    buf0, buf1, coef, outbox,
    halo_send, halo_recv, mem_send, mem_recv, own_sem,
):
    s = lax.axis_index("space")
    m = lax.axis_index("mem")
    nxt = lax.rem(s + 1, strips)
    prv = lax.rem(s + strips - 1, strips)
    rows = members.shape[1]
    width = members.shape[2]
    barrier = pltpu.get_barrier_semaphore()
    for other in (prv, nxt):
        pl.semaphore_signal(barrier, inc=1, device_id={"space": other}, device_id_type=MESH)
    for step in range(1, groups):
        peer = lax.rem(m + step, groups)
        pl.semaphore_signal(barrier, inc=1, device_id={"mem": peer}, device_id_type=MESH)

    def fill(r):
        ocean = land[pl.ds(r, 1), :].astype(f32)
        coef[3 + r, 0:1, :] = 0.5 * flow_east[pl.ds(r, 1), :]
        coef[3 + r, 1:2, :] = 0.5 * flow_north[pl.ds(r, 1), :]
        coef[3 + r, 2:3, :] = mixing[pl.ds(r, 1), :]
        coef[3 + r, 3:4, :] = ocean
        buf0[STEPS + r] = members[:, r, :] * ocean

    for r in range(STEPS):
        fill(r)
    for r in range(rows - STEPS, rows):
        fill(r)
    pl.semaphore_wait(barrier, 2 + groups - 1)

    def to(k, src, dst, other):
        return pltpu.make_async_remote_copy(
            src_ref=src, dst_ref=dst, send_sem=halo_send.at[k], recv_sem=halo_recv.at[k],
            device_id={"space": other}, device_id_type=MESH,
        )

    last = STEPS + rows
    halo = [
        to(0, buf0.at[pl.ds(rows, STEPS)], buf0.at[pl.ds(0, STEPS)], nxt),
        to(1, buf0.at[pl.ds(STEPS, STEPS)], buf0.at[pl.ds(last, STEPS)], prv),
        to(2, coef.at[pl.ds(rows, 3)], coef.at[pl.ds(0, 3)], nxt),
        to(3, coef.at[pl.ds(3, 3)], coef.at[pl.ds(3 + rows, 3)], prv),
        to(4, lists, lists_prev, nxt),
        to(5, lists, lists_next, prv),
    ]
    for copy in halo:
        copy.start()
    for r in range(STEPS, rows - STEPS):
        fill(r)
    for copy in halo:
        copy.wait_recv()

    @pl.when(s == 0)
    def _():
        buf0[pl.ds(0, STEPS)] = jnp.zeros((STEPS, 8, width), f32)
        coef[pl.ds(0, 3)] = jnp.zeros((3, 4, width), f32)
        lists_prev[...] = jnp.full(lists_prev.shape, -(1 << 20), i32)

    @pl.when(s == strips - 1)
    def _():
        buf0[pl.ds(last, STEPS)] = jnp.zeros((STEPS, 8, width), f32)
        coef[pl.ds(3 + rows, 3)] = jnp.zeros((3, 4, width), f32)
        lists_next[...] = jnp.full(lists_next.shape, -(1 << 20), i32)

    for copy in halo:
        copy.wait_send()

    def advance(src, i):
        c = src[i]
        n = src[i + 1]
        so = src[i - 1]
        e = pltpu.roll(c, width - 1, 1)
        w = pltpu.roll(c, 1, 1)
        fe = coef[i - 1, 0:1, :]
        fn = coef[i - 1, 1:2, :]
        mx = coef[i - 1, 2:3, :]
        oc = coef[i - 1, 3:4, :]
        carried = fe * (e - w) + fn * (n - so)
        spread = e + w + n + so - 4.0 * c
        return oc * (c - carried + mx * spread)

    bufs = (buf0, buf1)
    for step in range(STEPS - 1):
        src, dst = bufs[step % 2], bufs[(step + 1) % 2]

        def one(i, _, src=src, dst=dst):
            dst[i] = advance(src, i)
            return 0

        lax.fori_loop(step + 1, 2 * STEPS + rows - 1 - step, one, 0)
    src = bufs[(STEPS - 1) % 2]
    lane = lax.broadcasted_iota(i32, (8, TW), 1)

    def final(g, _):
        packed = [jnp.zeros((8, TW), f32) for _ in range(groups)]
        for q in range(4):
            r = 4 * g + q
            value = advance(src, STEPS + r)
            blocks = [value[:, b * TW : (b + 1) * TW] for b in range(groups)]
            for b in range(groups):
                outbox[b, r] = blocks[b]
                both = jnp.where(lane < EDGE, blocks[(b + 1) % groups], blocks[(b - 1) % groups])
                turned = pltpu.roll(both, (32 * q + EDGE) % TW, 1)
                packed[b] = jnp.where(lane // 32 == q, turned, packed[b])
        for b in range(groups):
            outbox[b, rows + g] = packed[b]
        return 0

    lax.fori_loop(0, rows // 4, final, 0)
    mine = window.at[:, pl.ds(pl.multiple_of(8 * m, 8), 8), :]
    copies = []
    for k, step in enumerate((4, 3, 5, 2, 6, 7, 1)):
        peer = lax.rem(m + step, groups)
        copy = pltpu.make_async_remote_copy(
            src_ref=outbox.at[peer], dst_ref=mine, send_sem=mem_send.at[k], recv_sem=mem_recv.at[k],
            device_id={"mem": peer}, device_id_type=MESH,
        )
        copy.start()
        copies.append(copy)
    own = pltpu.make_async_copy(outbox.at[m], mine, own_sem)
    own.start()
    own.wait()
    for copy in copies:
        copy.wait()


def forecast(members, flow_east, flow_north, mixing, land, lists, strips, groups):
    rows, width = members.shape[1:]
    packed_rows = rows + rows // 4
    return pl.pallas_call(
        functools.partial(forecast_kernel, strips, groups),
        name="forecast",
        out_shape=[
            jax.ShapeDtypeStruct((packed_rows, 8 * groups, TW), f32),
            jax.ShapeDtypeStruct(lists.shape, i32),
            jax.ShapeDtypeStruct(lists.shape, i32),
        ],
        in_specs=[pl.BlockSpec(memory_space=VMEM)] * 6,
        out_specs=[pl.BlockSpec(memory_space=VMEM)] * 3,
        scratch_shapes=[
            VMEM((rows + 2 * STEPS, 8, width), f32),
            VMEM((rows + 2 * STEPS, 8, width), f32),
            VMEM((rows + 6, 4, width), f32),
            VMEM((groups, packed_rows, 8, TW), f32),
            pltpu.SemaphoreType.DMA((6,)),
            pltpu.SemaphoreType.DMA((6,)),
            pltpu.SemaphoreType.DMA((groups - 1,)),
            pltpu.SemaphoreType.DMA((groups - 1,)),
            pltpu.SemaphoreType.DMA,
        ],
        compiler_params=pltpu.CompilerParams(
            collective_id=0, has_side_effects=True, vmem_limit_bytes=60 * 1024 * 1024
        ),
    )(members, flow_east, flow_north, mixing, land, lists)


def weight_kernel(
    width, per_strip, block_ref, lists_prev, lists, lists_next, cells, values, noises,
    weight, forced, place_ref, row_ref, w_ref, u_ref,
):
    chunks = per_strip // TW
    rows = lists.shape[0]
    block = block_ref[0]
    start = block * TW
    middle = start.astype(f32) + (TW - 1) / 2.0
    lane_rows = lax.broadcasted_iota(i32, (8, TW), 0)
    for d, source in enumerate((lists_prev, lists, lists_next)):
        for half in range(rows // 8):
            for side in range(lists.shape[1] // TW):
                entry = source[8 * half : 8 * half + 8, side * TW : (side + 1) * TW]
                j = entry + (d - 2) * per_strip
                usable = (j >= 0) & (j < per_strip)
                j = jnp.where(usable, j, 0)
                low = j & (TW - 1)
                high = j >> 7
                cell = jnp.zeros((8, TW), i32)
                value = jnp.zeros((8, TW), f32)
                noise = jnp.ones((8, TW), f32)
                for c in range(chunks):
                    here = high == c

                    def pick(table, c=c, low=low):
                        full = jnp.broadcast_to(table[c : c + 1, :], (8, TW))
                        return jnp.take_along_axis(full, low, axis=1, mode="promise_in_bounds")

                    cell = jnp.where(here, pick(cells), cell)
                    value = jnp.where(here, pick(values), value)
                    noise = jnp.where(here, pick(noises), noise)
                row = cell // width
                col = cell % width
                tile_row = lane_rows + (8 * half + (d - 1) * rows)
                dy = (row - tile_row).astype(f32)
                a = jnp.abs(col.astype(f32) - middle)
                a = jnp.minimum(a, float(width) - a)
                dx = jnp.maximum(a - (TW - 1) / 2.0, 0.0)
                distance = jnp.sqrt(dx * dx + dy * dy)
                w = jnp.where(usable, gaspari(distance / RLOC) / noise, 0.0)
                p = (col - start) & (width - 1)
                edge = jnp.where(p < TW + EDGE, p - TW + EDGE, p - (width - EDGE))
                edge = TW + 32 * (row & 3) + edge
                near = (p < TW + EDGE) | (p >= width - EDGE)
                place = jnp.where(p < TW, p, jnp.where(near, edge, -1))
                at = (pl.ds(rows * d + 8 * half, 8), pl.ds(side * TW, TW))
                place_ref[at] = place
                row_ref[at] = row
                w_ref[at] = w
                u_ref[at] = w * value

    slots = lists.shape[1]
    cell_iota = lax.broadcasted_iota(i32, (2 * TW, slots), 0)
    row_iota = lax.broadcasted_iota(i32, (rows, slots), 0)
    quad_iota = lax.broadcasted_iota(i32, (4, slots), 0)

    def one(t, _):
        place = place_ref[pl.ds(t, 1), :]
        row = row_ref[pl.ds(t, 1), :]
        w = w_ref[pl.ds(t, 1), :]
        u = u_ref[pl.ds(t, 1), :]
        hot = jnp.where(cell_iota == place, 1.0, 0.0).astype(bf16)
        parts = []
        for x in (w, u):
            high = x.astype(bf16).astype(f32)
            parts += [high, x - high]
        main = [jnp.where(row_iota == row, x, 0.0) for x in parts]
        quad = [jnp.where(quad_iota == row // 4, x, 0.0) for x in parts]
        both = jnp.concatenate(quad, axis=0)
        lhs = jnp.concatenate(main + [both], axis=0).astype(bf16)
        out = dot_nt(lhs, hot)
        weight[t, 0:rows, :] = out[0:rows, :TW] + out[rows : 2 * rows, :TW]
        forced[t, 0:rows, :] = out[2 * rows : 3 * rows, :TW] + out[3 * rows : 4 * rows, :TW]
        e = out[4 * rows :, TW:]
        weight[t, rows : rows + 4, :] = e[0:4] + e[4:8]
        forced[t, rows : rows + 4, :] = e[8:12] + e[12:16]
        return 0

    lax.fori_loop(0, 3 * rows, one, 0, unroll=4)


def weights(block, lists_prev, lists, lists_next, cells, values, noises, width):
    rows, slots = lists.shape
    per_strip = cells.shape[0]
    packed_rows = rows + rows // 4
    tables = [x.reshape(per_strip // TW, TW) for x in (cells, values, noises)]
    return pl.pallas_call(
        functools.partial(weight_kernel, width, per_strip),
        name="weights",
        out_shape=[jax.ShapeDtypeStruct((3 * rows, packed_rows, TW), f32)] * 2,
        in_specs=[pl.BlockSpec(memory_space=pltpu.SMEM)] + [pl.BlockSpec(memory_space=VMEM)] * 6,
        out_specs=[pl.BlockSpec(memory_space=VMEM)] * 2,
        scratch_shapes=[
            VMEM((3 * rows, slots), i32),
            VMEM((3 * rows, slots), i32),
            VMEM((3 * rows, slots), f32),
            VMEM((3 * rows, slots), f32),
        ],
        compiler_params=pltpu.CompilerParams(vmem_limit_bytes=60 * 1024 * 1024),
    )(block, lists_prev, lists, lists_next, *tables)


def gram_kernel(rows, window, weight, forced, gram, forcing, centred, hilo, dref):
    packed_rows, count, _ = window.shape
    tiles = packed_rows // 2
    for i in range(packed_rows):
        x = window[i]
        mean = jnp.sum(x, axis=0, keepdims=True) / count
        x = x - mean
        centred[i] = x
        at = pl.ds((i % 2) * TW, TW)
        high, low = split(x)
        hilo[i // 2, 0:count, at] = high
        hilo[i // 2, count : 2 * count, at] = low
        dref[:, i * TW : (i + 1) * TW] = forced[:, i, :] - weight[:, i, :] * mean
    total = jnp.zeros((2 * 3 * rows, 2 * count), f32)
    for k in range(tiles):
        high, low = split(dref[:, k * 2 * TW : (k + 1) * 2 * TW])
        total += dot_nt(jnp.concatenate([high, low], axis=0), hilo[k])
    total = total[: 3 * rows] + total[3 * rows :]
    forcing[...] = total + pltpu.roll(total, count, 1)

    def tile(t, need):
        acc = None
        for k in need:
            x = jnp.concatenate([centred[2 * k], centred[2 * k + 1]], axis=1)
            w = jnp.concatenate(
                [weight[t, 2 * k : 2 * k + 1, :], weight[t, 2 * k + 1 : 2 * k + 2, :]], axis=1
            )
            high, low = split(x * w)
            part = dot_nt(jnp.concatenate([high, low], axis=0), hilo[k])
            acc = part if acc is None else acc + part
        acc = acc[:count] + acc[count:]
        return acc + pltpu.roll(acc, count, 1)

    left = lax.broadcasted_iota(i32, (count, 2 * count), 1) < count
    main = rows // 2
    quarter = rows // 4

    for j in range(4):
        need = {
            1: tuple(range(tiles)),
            2: tuple(range(2 * j, main)) + ((main, main + 1) if j < 2 else (main + 1,)),
            0: tuple(range(0, 2 * j + 2)) + ((main,) if j < 2 else (main, main + 1)),
        }

        def pair(h, _, j=j, need=need):
            r = quarter * j + 2 * h
            for d in (0, 2, 1):
                a = tile(rows * d + r, need[d])
                b = tile(rows * d + r + 1, need[d])
                gram[4 * d + j, :, pl.ds(pl.multiple_of(h * 2 * count, 2 * count), 2 * count)] = jnp.where(left, a, b)
            return 0

        lax.fori_loop(0, 2, pair, 0)


def grams(window, weight, forced, rows):
    packed_rows, count, _ = window.shape
    return pl.pallas_call(
        functools.partial(gram_kernel, rows),
        name="grams",
        out_shape=[
            jax.ShapeDtypeStruct((12, count, 4 * count), f32),
            jax.ShapeDtypeStruct((3 * rows, 2 * count), f32),
        ],
        in_specs=[pl.BlockSpec(memory_space=VMEM)] * 3,
        out_specs=[pl.BlockSpec(memory_space=VMEM)] * 2,
        scratch_shapes=[
            VMEM((packed_rows, count, TW), f32),
            VMEM((packed_rows // 2, 2 * count, 2 * TW), bf16),
            VMEM((3 * rows, packed_rows * TW), f32),
        ],
        compiler_params=pltpu.CompilerParams(vmem_limit_bytes=60 * 1024 * 1024),
    )(window, weight, forced)


def share_kernel(strips, rows, gram, forcing, total, force, got_g, got_f, send, recv):
    s = lax.axis_index("space")
    nxt = lax.rem(s + 1, strips)
    prv = lax.rem(s + strips - 1, strips)
    barrier = pltpu.get_barrier_semaphore()
    for other in (prv, nxt):
        pl.semaphore_signal(barrier, inc=1, device_id={"space": other}, device_id_type=MESH)
    pl.semaphore_wait(barrier, 2)

    def to(k, src, dst, other):
        return pltpu.make_async_remote_copy(
            src_ref=src, dst_ref=dst, send_sem=send.at[k], recv_sem=recv.at[k],
            device_id={"space": other}, device_id_type=MESH,
        )

    copies = [
        to(0, gram.at[pl.ds(8, 4)], got_g.at[0], nxt),
        to(1, gram.at[pl.ds(0, 4)], got_g.at[1], prv),
        to(2, forcing.at[pl.ds(2 * rows, rows)], got_f.at[0], nxt),
        to(3, forcing.at[pl.ds(0, rows)], got_f.at[1], prv),
    ]
    for copy in copies:
        copy.start()
    total[...] = gram[pl.ds(4, 4)]
    force[...] = forcing[pl.ds(rows, rows)]
    for copy in copies:
        copy.wait()

    @pl.when(s > 0)
    def _():
        total[...] += got_g[0]
        force[...] += got_f[0]

    @pl.when(s < strips - 1)
    def _():
        total[...] += got_g[1]
        force[...] += got_f[1]


def share(gram, forcing, strips, rows):
    _, count, lanes = gram.shape
    return pl.pallas_call(
        functools.partial(share_kernel, strips, rows),
        name="share",
        out_shape=[
            jax.ShapeDtypeStruct((4, count, lanes), f32),
            jax.ShapeDtypeStruct((rows, forcing.shape[1]), f32),
        ],
        in_specs=[pl.BlockSpec(memory_space=VMEM)] * 2,
        out_specs=[pl.BlockSpec(memory_space=VMEM)] * 2,
        scratch_shapes=[
            VMEM((2, 4, count, lanes), f32),
            VMEM((2, rows, forcing.shape[1]), f32),
            pltpu.SemaphoreType.DMA((4,)),
            pltpu.SemaphoreType.DMA((4,)),
        ],
        compiler_params=pltpu.CompilerParams(collective_id=1, has_side_effects=True),
    )(gram, forcing)


def analysis_kernel(rows, gram, force, window, out):
    count = gram.shape[1]
    lanes = gram.shape[2]
    per = lanes // count
    row_of = lax.broadcasted_iota(i32, (count, lanes), 0)
    lane_of = lax.broadcasted_iota(i32, (count, lanes), 1)
    eye = jnp.where(row_of == lane_of % count, 1.0, 0.0).astype(f32)
    seg_row = lax.broadcasted_iota(i32, (lanes, lanes), 0) // count
    seg_col = lax.broadcasted_iota(i32, (lanes, lanes), 1) // count
    diag = seg_row == seg_col
    diag_one = jnp.where(diag, 1.0, 0.0).astype(bf16)

    def blocked(x):
        zero = jnp.zeros((), bf16)
        return jnp.where(diag, jnp.concatenate([x] * per, axis=0), zero)

    def parts(x):
        high, low = split(x)
        return (high, low), (blocked(high), blocked(low))

    def mul(a, b):
        (ah, al), (bh, bl) = a, b
        return dot_nn(ah, bh) + dot_nn(al, bh) + dot_nn(ah, bl)

    quads = rows // per
    z, r, scale = [], [], []
    for g in range(quads):
        b = eye + gram[g] / (count - 1)
        sq = jnp.sum(b * b, axis=0, keepdims=True)
        h1 = sq.astype(bf16)
        rest = sq - h1.astype(f32)
        h2 = rest.astype(bf16)
        h3 = (rest - h2.astype(f32)).astype(bf16)
        stacked = jnp.concatenate([jnp.broadcast_to(h, (16, lanes)) for h in (h1, h2, h3)], axis=0)
        sums = dot_nn(stacked, diag_one)
        frob = jnp.sqrt(sums[0:1] + sums[16:17] + sums[32:33])
        z.append(b / frob)
        scale.append(jnp.sqrt(frob))
    for step in range(NSITER):
        for g in range(quads):
            zl, zr = parts(z[g])
            if step == 0:
                f = 1.5 * eye - 0.5 * z[g]
                fl, _ = parts(f)
                r.append(f)
                z[g] = mul(fl, zr)
                continue
            rl, rr = parts(r[g])
            f = 1.5 * eye - 0.5 * mul(rl, zr)
            fl, _ = parts(f)
            if step < NSITER - 1:
                z[g] = mul(fl, zr)
            r[g] = mul(fl, rr)
    low_half = lax.broadcasted_iota(i32, (count, 2 * count), 1) < count
    for g in range(quads):
        t = r[g] / scale[g]
        (th, tl), tr = parts(t)
        vec = jnp.broadcast_to(force[g : g + 1, :], (16, lanes))
        vec = mul(split(vec), tr)
        vec = mul(split(vec), tr) / (count - 1)
        mix = t + vec[0:1]
        for h in range(per // 2):
            two = mix[:, h * 2 * count : (h + 1) * 2 * count]
            row0 = per * g + 2 * h
            fields, means = [], []
            for q in range(2):
                x = window[row0 + q]
                mean = jnp.sum(x, axis=0, keepdims=True) / count
                fields.append(x - mean)
                means.append(mean)
            xh, xl = split(jnp.concatenate(fields, axis=0))
            for q in range(2):
                keep = low_half if q == 0 else jnp.logical_not(low_half)
                lh, ll = split(jnp.where(keep, two, 0.0))
                out[:, row0 + q, :] = means[q] + (dot_nn(lh, xh) + dot_nn(ll, xh) + dot_nn(lh, xl))


def analyse(gram, force, window, rows):
    count = gram.shape[1]
    return pl.pallas_call(
        functools.partial(analysis_kernel, rows),
        name="analysis",
        out_shape=jax.ShapeDtypeStruct((count, rows, TW), f32),
        in_specs=[pl.BlockSpec(memory_space=VMEM)] * 3,
        out_specs=pl.BlockSpec(memory_space=VMEM),
        compiler_params=pltpu.CompilerParams(vmem_limit_bytes=60 * 1024 * 1024),
    )(gram, force, window)


def body(strips, groups, members, flow_east, flow_north, mixing, land_mask, sensor_cell,
         sensor_value, sensor_noise, tile_lists, tile_counts):
    rows, width = members.shape[1:]
    slot = jnp.arange(tile_lists.shape[2], dtype=i32)
    lists = jnp.where(slot[None, :] < tile_counts, tile_lists[:, 0, :], -(1 << 20))
    block = lax.axis_index("mem").astype(i32).reshape(1)
    window, lists_prev, lists_next = forecast(
        members, flow_east, flow_north, mixing, land_mask, lists, strips, groups
    )
    weight, forced = weights(
        block, lists_prev, lists, lists_next, sensor_cell, sensor_value, sensor_noise, width
    )
    gram, forcing = grams(window, weight, forced, rows)
    total, force = share(gram, forcing, strips, rows)
    count = window.shape[1]
    force = force[:, :count].reshape(rows // 4, 4 * count)
    return analyse(total, force, window, rows)


def solution(mesh):
    strips, groups = mesh.shape["space"], mesh.shape["mem"]
    in_specs = (
        P("mem", "space", None),
        P("space", None),
        P("space", None),
        P("space", None),
        P("space", None),
        P("space"),
        P("space"),
        P("space"),
        P("space", "mem", None),
        P("space", "mem"),
    )
    return jax.shard_map(
        functools.partial(body, strips, groups),
        mesh=mesh,
        in_specs=in_specs,
        out_specs=P(None, "space", "mem"),
        check_vma=False,
    )
```

```python
import functools

import jax
import jax.numpy as jnp
from jax import lax
from jax.experimental import pallas as pl
from jax.experimental.pallas import tpu as pltpu
from jax.sharding import PartitionSpec as P

TW = 128
STEPS = 4
NSITER = 8
RLOC = 8
EDGE = 16
MESH = pl.DeviceIdType.MESH
VMEM = pltpu.VMEM
f32 = jnp.float32
bf16 = jnp.bfloat16
i32 = jnp.int32


def split(x):
    high = x.astype(bf16)
    return high, (x - high.astype(f32)).astype(bf16)


def dot_nt(a, b):
    return lax.dot_general(a, b, (((1,), (1,)), ((), ())), preferred_element_type=f32)


def dot_nn(a, b):
    return jnp.dot(a, b, preferred_element_type=f32)


def gaspari(ratio):
    capped = jnp.maximum(ratio, 1.0)
    inner = (((-0.25 * ratio + 0.5) * ratio + 0.625) * ratio - 5.0 / 3.0) * ratio * ratio + 1.0
    outer = (
        ((((ratio / 12.0 - 0.5) * ratio + 0.625) * ratio + 5.0 / 3.0) * ratio - 5.0) * ratio
        + 4.0
        - 2.0 / (3.0 * capped)
    )
    return jnp.where(ratio <= 1.0, inner, jnp.where(ratio <= 2.0, outer, 0.0))


def cycle_kernel(
    strips, groups,
    members, flow_east, flow_north, mixing, land, tile_lists, tile_counts, cells, values, noises,
    window, total,
    buf0, buf1, coef, outbox, lists, place_ref, row_ref, w_ref, u_ref,
    weight, forced, centred, means, hilo, to_next, to_prev, got,
    halo_send, halo_recv, mem_send, mem_recv, own_sem,
    next_send, next_recv, prev_send, prev_recv,
):
    s = lax.axis_index("space")
    m = lax.axis_index("mem")
    nxt = lax.rem(s + 1, strips)
    prv = lax.rem(s + strips - 1, strips)
    rows = members.shape[1]
    width = members.shape[2]
    slots = tile_lists.shape[2]
    chunks = cells.shape[0]
    per_strip = chunks * TW
    count = 8 * groups
    barrier = pltpu.get_barrier_semaphore()
    for other in (prv, nxt):
        pl.semaphore_signal(barrier, inc=1, device_id={"space": other}, device_id_type=MESH)
    for step in range(1, groups):
        peer = lax.rem(m + step, groups)
        pl.semaphore_signal(barrier, inc=1, device_id={"mem": peer}, device_id_type=MESH)

    def fill(r):
        ocean = land[pl.ds(r, 1), :].astype(f32)
        coef[3 + r, 0:1, :] = 0.5 * flow_east[pl.ds(r, 1), :]
        coef[3 + r, 1:2, :] = 0.5 * flow_north[pl.ds(r, 1), :]
        coef[3 + r, 2:3, :] = mixing[pl.ds(r, 1), :]
        coef[3 + r, 3:4, :] = ocean
        buf0[STEPS + r] = members[:, r, :] * ocean

    for r in range(STEPS):
        fill(r)
    for r in range(rows - STEPS, rows):
        fill(r)
    slot = lax.broadcasted_iota(i32, (rows, slots), 1)
    lists[pl.ds(rows, rows)] = jnp.where(slot < tile_counts[...], tile_lists[:, 0, :], -(1 << 20))
    pl.semaphore_wait(barrier, 2 + groups - 1)

    def to(k, src, dst, other, send=halo_send, recv=halo_recv):
        return pltpu.make_async_remote_copy(
            src_ref=src, dst_ref=dst, send_sem=send.at[k], recv_sem=recv.at[k],
            device_id={"space": other}, device_id_type=MESH,
        )

    last = STEPS + rows
    mine_l = lists.at[pl.ds(rows, rows)]
    halo = [
        to(0, buf0.at[pl.ds(rows, STEPS)], buf0.at[pl.ds(0, STEPS)], nxt),
        to(1, buf0.at[pl.ds(STEPS, STEPS)], buf0.at[pl.ds(last, STEPS)], prv),
        to(2, coef.at[pl.ds(rows, 3)], coef.at[pl.ds(0, 3)], nxt),
        to(3, coef.at[pl.ds(3, 3)], coef.at[pl.ds(3 + rows, 3)], prv),
        to(4, mine_l, lists.at[pl.ds(0, rows)], nxt),
        to(5, mine_l, lists.at[pl.ds(2 * rows, rows)], prv),
    ]
    for copy in halo:
        copy.start()
    for r in range(STEPS, rows - STEPS):
        fill(r)

    start = m * TW
    middle = start.astype(f32) + (TW - 1) / 2.0
    lane_rows = lax.broadcasted_iota(i32, (8, TW), 0)

    def attributes(d):
        for half in range(rows // 8):
            for side in range(slots // TW):
                at = (pl.ds(pl.multiple_of(rows * d + 8 * half, 8), 8), pl.ds(side * TW, TW))
                j = lists[at] + (d - 2) * per_strip
                usable = (j >= 0) & (j < per_strip)
                j = jnp.where(usable, j, 0)
                low = j & (TW - 1)
                high = j >> 7
                cell = jnp.zeros((8, TW), i32)
                value = jnp.zeros((8, TW), f32)
                noise = jnp.ones((8, TW), f32)
                for c in range(chunks):
                    here = high == c

                    def pick(table, c=c, low=low):
                        full = jnp.broadcast_to(table[c : c + 1, :], (8, TW))
                        return jnp.take_along_axis(full, low, axis=1, mode="promise_in_bounds")

                    cell = jnp.where(here, pick(cells), cell)
                    value = jnp.where(here, pick(values), value)
                    noise = jnp.where(here, pick(noises), noise)
                shift = width.bit_length() - 1
                row = cell >> shift
                col = cell & (width - 1)
                tile_row = lane_rows + (8 * half + (d - 1) * rows)
                dy = (row - tile_row).astype(f32)
                a = jnp.abs(col.astype(f32) - middle)
                a = jnp.minimum(a, float(width) - a)
                dx = jnp.maximum(a - (TW - 1) / 2.0, 0.0)
                distance = jnp.sqrt(dx * dx + dy * dy)
                w = jnp.where(usable, gaspari(distance / RLOC) / noise, 0.0)
                p = (col - start) & (width - 1)
                edge = jnp.where(p < TW + EDGE, p - TW + EDGE, p - (width - EDGE))
                edge = TW + 32 * (row & 3) + edge
                near = (p < TW + EDGE) | (p >= width - EDGE)
                place_ref[at] = jnp.where(p < TW, p, jnp.where(near, edge, -1))
                row_ref[at] = row
                w_ref[at] = w
                u_ref[at] = w * value

    half = rows // 2
    cell_iota = lax.broadcasted_iota(i32, (2 * TW, slots), 0)
    ri = lax.broadcasted_iota(i32, (rows, slots), 0)
    row_iota = 2 * (ri & (half - 1)) + ri // half
    qi = lax.broadcasted_iota(i32, (4, slots), 0)
    quad_iota = 2 * (qi & 1) + (qi >> 1)

    def scatter(t):
        place = place_ref[pl.ds(t, 1), :]
        row = row_ref[pl.ds(t, 1), :]
        hot = jnp.where(cell_iota == place, 1.0, 0.0).astype(bf16)
        parts = []
        for x in (w_ref[pl.ds(t, 1), :], u_ref[pl.ds(t, 1), :]):
            high = x.astype(bf16).astype(f32)
            parts += [high, x - high]
        main = [jnp.where(row_iota == row, x, 0.0) for x in parts]
        quad = [jnp.where(quad_iota == (row >> 2), x, 0.0) for x in parts]
        both = jnp.concatenate(quad, axis=0)
        lhs = jnp.concatenate(main + [both], axis=0).astype(bf16)
        out = dot_nt(lhs, hot)
        for k, ref in ((0, weight), (2, forced)):
            x = out[k * rows : (k + 1) * rows, :TW] + out[(k + 1) * rows : (k + 2) * rows, :TW]
            ref[t, 0:half, 0:TW] = x[0:half]
            ref[t, 0:half, TW : 2 * TW] = x[half:rows]
            at = 4 * rows + 4 * k
            e = out[at : at + 4, TW:] + out[at + 4 : at + 8, TW:]
            ref[t, half : half + 2, 0:TW] = e[0:2]
            ref[t, half : half + 2, TW : 2 * TW] = e[2:4]

    attributes(jnp.int32(1))

    def scatter_own(i, _):
        for q in range(4):
            scatter(rows + 4 * i + q)
        return 0

    lax.fori_loop(0, rows // 4, scatter_own, 0)

    for copy in halo:
        copy.wait_recv()

    @pl.when(s == 0)
    def _():
        buf0[pl.ds(0, STEPS)] = jnp.zeros((STEPS, 8, width), f32)
        coef[pl.ds(0, 3)] = jnp.zeros((3, 4, width), f32)
        lists[pl.ds(0, rows)] = jnp.full((rows, slots), -(1 << 20), i32)

    @pl.when(s == strips - 1)
    def _():
        buf0[pl.ds(last, STEPS)] = jnp.zeros((STEPS, 8, width), f32)
        coef[pl.ds(3 + rows, 3)] = jnp.zeros((3, 4, width), f32)
        lists[pl.ds(2 * rows, rows)] = jnp.full((rows, slots), -(1 << 20), i32)

    for copy in halo:
        copy.wait_send()

    def advance(src, i):
        c = src[i]
        n = src[i + 1]
        so = src[i - 1]
        e = pltpu.roll(c, width - 1, 1)
        w = pltpu.roll(c, 1, 1)
        fe = coef[i - 1, 0:1, :]
        fn = coef[i - 1, 1:2, :]
        mx = coef[i - 1, 2:3, :]
        oc = coef[i - 1, 3:4, :]
        carried = fe * (e - w) + fn * (n - so)
        spread = e + w + n + so - 4.0 * c
        return oc * (c - carried + mx * spread)

    bufs = (buf0, buf1)
    for step in range(STEPS - 1):
        src, dst = bufs[step % 2], bufs[(step + 1) % 2]

        def one(i, _, src=src, dst=dst):
            dst[i] = advance(src, i)
            return 0

        lax.fori_loop(step + 1, 2 * STEPS + rows - 1 - step, one, 0)
    src = bufs[(STEPS - 1) % 2]
    lane = lax.broadcasted_iota(i32, (8, TW), 1)

    def final(g, _):
        packed = [jnp.zeros((8, TW), f32) for _ in range(groups)]
        for q in range(4):
            r = 4 * g + q
            value = advance(src, STEPS + r)
            blocks = [value[:, b * TW : (b + 1) * TW] for b in range(groups)]
            for b in range(groups):
                outbox[b, r] = blocks[b]
                both = jnp.where(lane < EDGE, blocks[(b + 1) % groups], blocks[(b - 1) % groups])
                turned = pltpu.roll(both, (32 * q + EDGE) % TW, 1)
                packed[b] = jnp.where(lane // 32 == q, turned, packed[b])
        for b in range(groups):
            outbox[b, rows + g] = packed[b]
        return 0

    lax.fori_loop(0, rows // 4, final, 0)
    mine = window.at[:, pl.ds(pl.multiple_of(8 * m, 8), 8), :]
    copies = []
    for k, step in enumerate((4, 3, 5, 2, 6, 7, 1)):
        peer = lax.rem(m + step, groups)
        copy = pltpu.make_async_remote_copy(
            src_ref=outbox.at[peer], dst_ref=mine, send_sem=mem_send.at[k], recv_sem=mem_recv.at[k],
            device_id={"mem": peer}, device_id_type=MESH,
        )
        copy.start()
        copies.append(copy)
    own = pltpu.make_async_copy(outbox.at[m], mine, own_sem)
    own.start()

    def attributes_far(i, _):
        attributes(2 * i)
        return 0

    lax.fori_loop(0, 2, attributes_far, 0)

    def scatter_far(i, _):
        for q in range(4):
            scatter(jnp.where(i < rows // 4, 4 * i, 4 * i + rows) + q)
        return 0

    lax.fori_loop(0, rows // 2, scatter_far, 0)
    own.wait()
    for copy in copies:
        copy.wait()

    packed_rows = window.shape[0]
    tiles = packed_rows // 2

    def centre(k, _):
        x = jnp.concatenate([window[2 * k], window[2 * k + 1]], axis=1)
        mean = jnp.sum(x, axis=0, keepdims=True) * (1.0 / count)
        x = x - mean
        centred[k] = x
        means[pl.ds(k, 1), :] = mean
        high, low = split(x)
        both = jnp.concatenate([high, low], axis=0)
        zero = jnp.zeros((2 * count, 2 * TW), bf16)
        hilo[k, 0, 0 : 2 * count, :] = both
        hilo[k, 0, 2 * count : 4 * count, :] = zero
        hilo[k, 1, 0 : 2 * count, :] = zero
        hilo[k, 1, 2 * count : 4 * count, :] = both
        return 0

    lax.fori_loop(0, tiles, centre, 0)

    def left(k, base, factor=None):
        x = centred[k]
        mean = means[pl.ds(k, 1), :]
        pieces, vectors = [], []
        for q in range(4):
            w = weight[base + q, pl.ds(k, 1), :]
            u = forced[base + q, pl.ds(k, 1), :]
            if factor is not None:
                w = w * factor
                u = u * factor
            high, low = split(x * w)
            pieces += [high, low]
            vectors.append(u - w * mean)
        v = jnp.concatenate(vectors + [jnp.zeros((4, 2 * TW), f32)], axis=0)
        top = v.astype(bf16).astype(f32)
        pieces.append(jnp.concatenate([top, v - top], axis=0).astype(bf16))
        return jnp.concatenate(pieces, axis=0)

    low_half = lax.broadcasted_iota(i32, (count, TW), 1) < count
    low_row = lax.broadcasted_iota(i32, (1, TW), 1) < count

    def store(ref, at, acc):
        folded = []
        for q in range(4):
            x = acc[2 * q * count : (2 * q + 1) * count] + acc[(2 * q + 1) * count : (2 * q + 2) * count]
            folded.append(x + pltpu.roll(x, count, 1))
        v = acc[8 * count : 8 * count + 8] + acc[8 * count + 8 : 8 * count + 16]
        v = v + pltpu.roll(v, count, 1)
        for h in range(2):
            lanes = slice(h * TW, (h + 1) * TW)
            ref[at, 0:count, lanes] = jnp.where(low_half, folded[2 * h], folded[2 * h + 1])
            row = jnp.where(low_row, v[2 * h : 2 * h + 1], v[2 * h + 1 : 2 * h + 2])
            ref[at, count : count + 8, lanes] = jnp.broadcast_to(row, (8, TW))

    main = rows // 2

    def ahead_copy(c):
        return to(c, to_next.at[c], got.at[0, c], nxt, next_send, next_recv)

    def behind_copy(c):
        return to(c, to_prev.at[c + 1], got.at[1, c], prv, prev_send, prev_recv)

    def far(c, _):
        nb = 2 * rows + 4 * c
        pb = 4 * (c - 1)
        acc = None

        def add(acc, k, base, sel, factor=None):
            part = dot_nt(left(k, base, factor), hilo[k, sel])
            return part if acc is None else acc + part

        for k in range(main):
            ahead = 2 * c <= k
            acc = add(acc, k, jnp.where(ahead, nb, pb), jnp.where(ahead, 0, 1))
        ahead = c < 4
        acc = add(acc, main + 1, jnp.where(ahead, nb, pb), jnp.where(ahead, 0, 1))
        behind = c >= 1
        acc = add(acc, main, jnp.where(behind, pb, nb), jnp.where(behind, 1, 0))
        factor = jnp.where((c == 1) | (c == 3), jnp.float32(1.0), jnp.float32(0.0))
        base = jnp.where(c == 1, nb, jnp.where(c == 3, pb, 0))
        acc = add(acc, jnp.where(c == 3, main + 1, main), base, jnp.where(c == 3, 1, 0), factor)
        store(to_next, c, acc[:, 0:TW])
        store(to_prev, c, acc[:, TW : 2 * TW])

        @pl.when(c < 4)
        def _():
            ahead_copy(c).start()

        @pl.when(c >= 1)
        def _():
            behind_copy(c - 1).start()

        return 0

    lax.fori_loop(0, 5, far, 0)

    def near(j, _):
        acc = None
        for k in range(tiles):
            part = dot_nt(left(k, rows + 4 * j), hilo[k, 0, 0 : 2 * count, :])
            acc = part if acc is None else acc + part
        store(total, j, acc)
        return 0

    lax.fori_loop(0, 4, near, 0)
    for c in range(4):
        ahead_copy(c).wait()
        behind_copy(c).wait()

    @pl.when(s > 0)
    def _():
        total[...] += got[0]

    @pl.when(s < strips - 1)
    def _():
        total[...] += got[1]


def cycle(members, flow_east, flow_north, mixing, land, lists, counts, cells, values, noises, strips, groups):
    rows, width = members.shape[1:]
    slots = lists.shape[2]
    packed_rows = rows + rows // 4
    tiles = packed_rows // 2
    count = 8 * groups
    tables = [x.reshape(-1, TW) for x in (cells, values, noises)]
    dma = pltpu.SemaphoreType.DMA
    return pl.pallas_call(
        functools.partial(cycle_kernel, strips, groups),
        name="cycle",
        out_shape=[
            jax.ShapeDtypeStruct((packed_rows, count, TW), f32),
            jax.ShapeDtypeStruct((4, count + 8, 4 * count), f32),
        ],
        in_specs=[pl.BlockSpec(memory_space=VMEM)] * 10,
        out_specs=[pl.BlockSpec(memory_space=VMEM)] * 2,
        scratch_shapes=[
            VMEM((rows + 2 * STEPS, 8, width), f32),
            VMEM((rows + 2 * STEPS, 8, width), f32),
            VMEM((rows + 6, 4, width), f32),
            VMEM((groups, packed_rows, 8, TW), f32),
            VMEM((3 * rows, slots), i32),
            VMEM((3 * rows, slots), i32),
            VMEM((3 * rows, slots), i32),
            VMEM((3 * rows, slots), f32),
            VMEM((3 * rows, slots), f32),
            VMEM((3 * rows, tiles, 2 * TW), f32),
            VMEM((3 * rows, tiles, 2 * TW), f32),
            VMEM((tiles, count, 2 * TW), f32),
            VMEM((tiles, 2 * TW), f32),
            VMEM((tiles, 2, 4 * count, 2 * TW), bf16),
            VMEM((5, count + 8, 4 * count), f32),
            VMEM((5, count + 8, 4 * count), f32),
            VMEM((2, 4, count + 8, 4 * count), f32),
            dma((6,)), dma((6,)), dma((groups - 1,)), dma((groups - 1,)), dma,
            dma((4,)), dma((4,)), dma((4,)), dma((4,)),
        ],
        compiler_params=pltpu.CompilerParams(
            collective_id=0, has_side_effects=True, vmem_limit_bytes=40 * 1024 * 1024
        ),
    )(members, flow_east, flow_north, mixing, land, lists, counts, *tables)


def analysis_kernel(gram, window, out, zs, rs, scales):
    quads, count, lanes = zs.shape
    per = lanes // count
    row_of = lax.broadcasted_iota(i32, (count, lanes), 0)
    lane_of = lax.broadcasted_iota(i32, (count, lanes), 1)
    eye = jnp.where(row_of == lane_of % count, 1.0, 0.0).astype(f32)
    seg_row = lax.broadcasted_iota(i32, (lanes, lanes), 0) // count
    seg_col = lax.broadcasted_iota(i32, (lanes, lanes), 1) // count
    diag = seg_row == seg_col
    diag_one = jnp.where(diag, 1.0, 0.0).astype(bf16)

    def blocked(x):
        return jnp.where(diag, jnp.concatenate([x] * per, axis=0), jnp.zeros((), bf16))

    def right(x):
        return blocked(x[0]), blocked(x[1])

    def mul(a, b):
        (ah, al), (bh, bl) = a, b
        n = ah.shape[0]
        p = dot_nn(jnp.concatenate([ah, al], axis=0), bh)
        return p[:n] + p[n:] + dot_nn(ah, bl)

    for g in range(quads):
        b = eye + gram[g, 0:count, :] / (count - 1)
        sq = jnp.sum(b * b, axis=0, keepdims=True)
        h1 = sq.astype(bf16)
        rest = sq - h1.astype(f32)
        h2 = rest.astype(bf16)
        h3 = (rest - h2.astype(f32)).astype(bf16)
        stacked = jnp.concatenate([jnp.broadcast_to(h, (16, lanes)) for h in (h1, h2, h3)], axis=0)
        sums = dot_nn(stacked, diag_one)
        frob = jnp.sqrt(sums[0:1] + sums[16:17] + sums[32:33])
        z = b / frob
        scales[pl.ds(g, 1), :] = jnp.sqrt(frob)
        f = 1.5 * eye - 0.5 * z
        rs[g] = f
        zs[g] = mul(split(f), right(split(z)))

    def step(i, _):
        for g in range(quads):
            r, zr = split(rs[g]), right(split(zs[g]))
            f = split(1.5 * eye - 0.5 * mul(r, zr))
            zs[g] = mul(f, zr)
            rs[g] = mul(f, right(r))
        return 0

    lax.fori_loop(0, NSITER - 2, step, 0)
    low_half = lax.broadcasted_iota(i32, (count, 2 * count), 1) < count

    for g in range(quads):
        r = split(rs[g])
        f = split(1.5 * eye - 0.5 * mul(r, right(split(zs[g]))))
        t = mul(f, right(r)) / scales[pl.ds(g, 1), :]
        tr = right(split(t))
        vec = jnp.broadcast_to(gram[g, count : count + 1, :], (16, lanes))
        vec = mul(split(vec), tr)
        vec = mul(split(vec), tr) / (count - 1)
        mix = t + vec[0:1]
        for h in range(per // 2):
            two = mix[:, h * 2 * count : (h + 1) * 2 * count]
            row0 = per * g + 2 * h
            fields, averages = [], []
            for q in range(2):
                x = window[row0 + q]
                mean = jnp.sum(x, axis=0, keepdims=True) * (1.0 / count)
                fields.append(x - mean)
                averages.append(mean)
            x = split(jnp.concatenate(fields, axis=0))
            lhs = jnp.concatenate([jnp.where(low_half, two, 0.0), jnp.where(low_half, 0.0, two)], axis=0)
            y = mul(split(lhs), x)
            for q in range(2):
                out[:, row0 + q, :] = averages[q] + y[q * count : (q + 1) * count]


def analyse(gram, window, rows):
    quads, _, lanes = gram.shape
    count = window.shape[1]
    return pl.pallas_call(
        analysis_kernel,
        name="analysis",
        out_shape=jax.ShapeDtypeStruct((count, rows, TW), f32),
        in_specs=[pl.BlockSpec(memory_space=VMEM)] * 2,
        out_specs=pl.BlockSpec(memory_space=VMEM),
        scratch_shapes=[
            VMEM((quads, count, lanes), f32),
            VMEM((quads, count, lanes), f32),
            VMEM((quads, lanes), f32),
        ],
        compiler_params=pltpu.CompilerParams(vmem_limit_bytes=16 * 1024 * 1024),
    )(gram, window)


def body(strips, groups, members, flow_east, flow_north, mixing, land_mask, sensor_cell,
         sensor_value, sensor_noise, tile_lists, tile_counts):
    window, total = cycle(
        members, flow_east, flow_north, mixing, land_mask, tile_lists, tile_counts,
        sensor_cell, sensor_value, sensor_noise, strips, groups,
    )
    return analyse(total, window, members.shape[1])


def solution(mesh):
    strips, groups = mesh.shape["space"], mesh.shape["mem"]
    in_specs = (
        P("mem", "space", None),
        P("space", None),
        P("space", None),
        P("space", None),
        P("space", None),
        P("space"),
        P("space"),
        P("space"),
        P("space", "mem", None),
        P("space", "mem"),
    )
    return jax.shard_map(
        functools.partial(body, strips, groups),
        mesh=mesh,
        in_specs=in_specs,
        out_specs=P(None, "space", "mem"),
        check_vma=False,
    )
```

```python
import functools

import jax
import jax.numpy as jnp
from jax import lax
from jax.experimental import pallas as pl
from jax.experimental.pallas import tpu as pltpu
from jax.sharding import PartitionSpec as P

TW = 128
STEPS = 4
NSITER = 8
RLOC = 8
EDGE = 16
MESH = pl.DeviceIdType.MESH
VMEM = pltpu.VMEM
f32 = jnp.float32
bf16 = jnp.bfloat16
i32 = jnp.int32


def split(x):
    high = x.astype(bf16)
    return high, (x - high.astype(f32)).astype(bf16)


def dot_nt(a, b):
    return lax.dot_general(a, b, (((1,), (1,)), ((), ())), preferred_element_type=f32)


def dot_nn(a, b):
    return jnp.dot(a, b, preferred_element_type=f32)


def gaspari(ratio):
    capped = jnp.maximum(ratio, 1.0)
    inner = (((-0.25 * ratio + 0.5) * ratio + 0.625) * ratio - 5.0 / 3.0) * ratio * ratio + 1.0
    outer = (
        ((((ratio / 12.0 - 0.5) * ratio + 0.625) * ratio + 5.0 / 3.0) * ratio - 5.0) * ratio
        + 4.0
        - 2.0 / (3.0 * capped)
    )
    return jnp.where(ratio <= 1.0, inner, jnp.where(ratio <= 2.0, outer, 0.0))


def cycle_kernel(
    strips, groups,
    members_h, east_h, north_h, mixing_h, land_h, lists_h, counts_h, cells_h, values_h, noises_h,
    centred, means, total,
    members, flow_east, flow_north, mixing, land, tile_lists, tile_counts, cells, values, noises,
    window, buf0, buf1, buf2, coef, outbox, lists, place_ref, row_ref, w_ref, u_ref,
    weight, forced, hilo, to_next, to_prev, got,
    load_sem, halo_send, halo_recv, mem_send, mem_recv, own_sem,
    next_send, next_recv, prev_send, prev_recv,
):
    loads = [
        pltpu.make_async_copy(src, dst, load_sem.at[k])
        for k, (src, dst) in enumerate((
            (members_h, members), (land_h, land), (east_h, flow_east), (north_h, flow_north),
            (mixing_h, mixing), (lists_h, tile_lists), (cells_h, cells), (values_h, values),
            (noises_h, noises), (counts_h, tile_counts),
        ))
    ]
    for copy in loads:
        copy.start()
    s = lax.axis_index("space")
    m = lax.axis_index("mem")
    nxt = lax.rem(s + 1, strips)
    prv = lax.rem(s + strips - 1, strips)
    rows = members.shape[1]
    width = members.shape[2]
    slots = tile_lists.shape[2]
    chunks = cells.shape[0]
    per_strip = chunks * TW
    count = 8 * groups
    barrier = pltpu.get_barrier_semaphore()
    for other in (prv, nxt):
        pl.semaphore_signal(barrier, inc=1, device_id={"space": other}, device_id_type=MESH)
    for step in range(1, groups):
        peer = lax.rem(m + step, groups)
        pl.semaphore_signal(barrier, inc=1, device_id={"mem": peer}, device_id_type=MESH)

    def fill(r):
        ocean = land[pl.ds(r, 1), :].astype(f32)
        coef[3 + r, 0:1, :] = 0.5 * flow_east[pl.ds(r, 1), :]
        coef[3 + r, 1:2, :] = 0.5 * flow_north[pl.ds(r, 1), :]
        coef[3 + r, 2:3, :] = mixing[pl.ds(r, 1), :]
        coef[3 + r, 3:4, :] = ocean
        buf0[STEPS + r] = members[:, r, :] * ocean

    for copy in loads:
        copy.wait()
    for r in range(STEPS):
        fill(r)
    for r in range(rows - STEPS, rows):
        fill(r)
    slot = lax.broadcasted_iota(i32, (rows, slots), 1)
    square = lax.broadcasted_iota(i32, (rows, rows), 0) == lax.broadcasted_iota(i32, (rows, rows), 1)
    used = jnp.where(square, jnp.broadcast_to(tile_counts[...].astype(f32), (rows, rows)), 0.0)
    used = jnp.sum(used, axis=1, keepdims=True)
    lists[pl.ds(rows, rows)] = jnp.where(slot.astype(f32) < used, tile_lists[:, 0, :], -(1 << 20))
    pl.semaphore_wait(barrier, 2 + groups - 1)

    def to(k, src, dst, other, send=halo_send, recv=halo_recv):
        return pltpu.make_async_remote_copy(
            src_ref=src, dst_ref=dst, send_sem=send.at[k], recv_sem=recv.at[k],
            device_id={"space": other}, device_id_type=MESH,
        )

    last = STEPS + rows
    mine_l = lists.at[pl.ds(rows, rows)]
    halo = [
        to(0, buf0.at[pl.ds(rows, STEPS)], buf0.at[pl.ds(0, STEPS)], nxt),
        to(1, buf0.at[pl.ds(STEPS, STEPS)], buf0.at[pl.ds(last, STEPS)], prv),
        to(2, coef.at[pl.ds(rows, 3)], coef.at[pl.ds(0, 3)], nxt),
        to(3, coef.at[pl.ds(3, 3)], coef.at[pl.ds(3 + rows, 3)], prv),
        to(4, mine_l, lists.at[pl.ds(0, rows)], nxt),
        to(5, mine_l, lists.at[pl.ds(2 * rows, rows)], prv),
    ]
    for copy in halo:
        copy.start()
    for r in range(STEPS, rows - STEPS):
        fill(r)

    start = m * TW
    middle = start.astype(f32) + (TW - 1) / 2.0
    lane_rows = lax.broadcasted_iota(i32, (8, TW), 0)

    def attributes(d):
        for half in range(rows // 8):
            for side in range(slots // TW):
                at = (pl.ds(pl.multiple_of(rows * d + 8 * half, 8), 8), pl.ds(side * TW, TW))
                j = lists[at] + (d - 2) * per_strip
                usable = (j >= 0) & (j < per_strip)
                j = jnp.where(usable, j, 0)
                low = j & (TW - 1)
                high = j >> 7
                cell = jnp.zeros((8, TW), i32)
                value = jnp.zeros((8, TW), f32)
                noise = jnp.ones((8, TW), f32)
                for c in range(chunks):
                    here = high == c

                    def pick(table, c=c, low=low):
                        full = jnp.broadcast_to(table[c : c + 1, :], (8, TW))
                        return jnp.take_along_axis(full, low, axis=1, mode="promise_in_bounds")

                    cell = jnp.where(here, pick(cells), cell)
                    value = jnp.where(here, pick(values), value)
                    noise = jnp.where(here, pick(noises), noise)
                shift = width.bit_length() - 1
                row = cell >> shift
                col = cell & (width - 1)
                tile_row = lane_rows + (8 * half + (d - 1) * rows)
                dy = (row - tile_row).astype(f32)
                a = jnp.abs(col.astype(f32) - middle)
                a = jnp.minimum(a, float(width) - a)
                dx = jnp.maximum(a - (TW - 1) / 2.0, 0.0)
                distance = jnp.sqrt(dx * dx + dy * dy)
                w = jnp.where(usable, gaspari(distance / RLOC) / noise, 0.0)
                p = (col - start) & (width - 1)
                edge = jnp.where(p < TW + EDGE, p - TW + EDGE, p - (width - EDGE))
                edge = TW + 32 * (row & 3) + edge
                near = (p < TW + EDGE) | (p >= width - EDGE)
                place_ref[at] = jnp.where(p < TW, p, jnp.where(near, edge, -1))
                row_ref[at] = row
                w_ref[at] = w
                u_ref[at] = w * value

    half = rows // 2
    cell_iota = lax.broadcasted_iota(i32, (2 * TW, slots), 0)
    ri = lax.broadcasted_iota(i32, (rows, slots), 0)
    row_iota = 2 * (ri & (half - 1)) + ri // half
    qi = lax.broadcasted_iota(i32, (4, slots), 0)
    quad_iota = 2 * (qi & 1) + (qi >> 1)

    def scatter(t):
        place = place_ref[pl.ds(t, 1), :]
        row = row_ref[pl.ds(t, 1), :]
        hot = jnp.where(cell_iota == place, 1.0, 0.0).astype(bf16)
        parts = []
        for x in (w_ref[pl.ds(t, 1), :], u_ref[pl.ds(t, 1), :]):
            high = x.astype(bf16).astype(f32)
            parts += [high, x - high]
        main = [jnp.where(row_iota == row, x, 0.0) for x in parts]
        quad = [jnp.where(quad_iota == (row >> 2), x, 0.0) for x in parts]
        both = jnp.concatenate(quad, axis=0)
        lhs = jnp.concatenate(main + [both], axis=0).astype(bf16)
        out = dot_nt(lhs, hot)
        for k, ref in ((0, weight), (2, forced)):
            x = out[k * rows : (k + 1) * rows, :TW] + out[(k + 1) * rows : (k + 2) * rows, :TW]
            at = 4 * rows + 4 * k
            e = out[at : at + 4, TW:] + out[at + 4 : at + 8, TW:]
            low, high = x[0:half], x[half:rows]
            part = half // 2
            ref[t, :, 0:TW] = jnp.concatenate([low[:part], e[0:1], low[part:], e[1:2]], axis=0)
            ref[t, :, TW : 2 * TW] = jnp.concatenate([high[:part], e[2:3], high[part:], e[3:4]], axis=0)

    attributes(jnp.int32(1))

    def scatter_own(i, _):
        for q in range(4):
            scatter(rows + 4 * i + q)
        return 0

    lax.fori_loop(0, rows // 4, scatter_own, 0)

    def advance(src, i):
        c = src[i]
        n = src[i + 1]
        so = src[i - 1]
        e = pltpu.roll(c, width - 1, 1)
        w = pltpu.roll(c, 1, 1)
        fe = coef[i - 1, 0:1, :]
        fn = coef[i - 1, 1:2, :]
        mx = coef[i - 1, 2:3, :]
        oc = coef[i - 1, 3:4, :]
        carried = fe * (e - w) + fn * (n - so)
        spread = e + w + n + so - 4.0 * c
        return oc * (c - carried + mx * spread)

    chain = (buf0, buf1, buf2, buf1)
    for step in range(STEPS - 1):
        src, dst = chain[step], chain[step + 1]

        def inner(i, _, src=src, dst=dst, first=STEPS + 1 + step):
            for q in range(2):
                dst[first + 2 * i + q] = advance(src, first + 2 * i + q)
            return 0

        lax.fori_loop(0, (rows - 2 - 2 * step) // 2, inner, 0)

    for copy in halo:
        copy.wait_recv()

    @pl.when(s == 0)
    def _():
        buf0[pl.ds(0, STEPS)] = jnp.zeros((STEPS, 8, width), f32)
        coef[pl.ds(0, 3)] = jnp.zeros((3, 4, width), f32)
        lists[pl.ds(0, rows)] = jnp.full((rows, slots), -(1 << 20), i32)

    @pl.when(s == strips - 1)
    def _():
        buf0[pl.ds(last, STEPS)] = jnp.zeros((STEPS, 8, width), f32)
        coef[pl.ds(3 + rows, 3)] = jnp.zeros((3, 4, width), f32)
        lists[pl.ds(2 * rows, rows)] = jnp.full((rows, slots), -(1 << 20), i32)

    for copy in halo:
        copy.wait_send()

    for step in range(STEPS - 1):
        src, dst = chain[step], chain[step + 1]

        def outer(i, _, src=src, dst=dst, low=step + 1, high=rows + STEPS - 1 - step):
            dst[low + i] = advance(src, low + i)
            dst[high + i] = advance(src, high + i)
            return 0

        lax.fori_loop(0, STEPS, outer, 0)
    src = chain[STEPS - 1]
    lane = lax.broadcasted_iota(i32, (8, TW), 1)

    packed_rows = window.shape[0]
    chunk = packed_rows // 2

    def final(g, _, shift=0):
        packed = [jnp.zeros((8, TW), f32) for _ in range(groups)]
        for q in range(4):
            r = 4 * g + q
            value = advance(src, STEPS + r)
            blocks = [value[:, b * TW : (b + 1) * TW] for b in range(groups)]
            for b in range(groups):
                outbox[b, r + shift] = blocks[b]
                both = jnp.where(lane < EDGE, blocks[(b + 1) % groups], blocks[(b - 1) % groups])
                turned = pltpu.roll(both, (32 * q + EDGE) % TW, 1)
                packed[b] = jnp.where(lane // 32 == q, turned, packed[b])
        for b in range(groups):
            outbox[b, rows // 2 + 4 * shift + g] = packed[b]
        return 0

    copies, own = [], []
    for part in range(2):
        lax.fori_loop(2 * part, 2 * part + 2, functools.partial(final, shift=2 * part), 0)
        here = pl.ds(chunk * part, chunk)
        mine = window.at[here, pl.ds(pl.multiple_of(8 * m, 8), 8), :]
        for k, step in enumerate((4, 3, 5, 2, 6, 7, 1)):
            peer = lax.rem(m + step, groups)
            at = part * (groups - 1) + k
            copy = pltpu.make_async_remote_copy(
                src_ref=outbox.at[peer, here], dst_ref=mine, send_sem=mem_send.at[at],
                recv_sem=mem_recv.at[at], device_id={"mem": peer}, device_id_type=MESH,
            )
            copy.start()
            copies.append(copy)
        own.append(pltpu.make_async_copy(outbox.at[m, here], mine, own_sem.at[part]))
        own[part].start()

    def attributes_far(i, _):
        attributes(2 * i)
        return 0

    lax.fori_loop(0, 2, attributes_far, 0)

    def scatter_far(i, _):
        for q in range(4):
            scatter(jnp.where(i < rows // 4, 4 * i, 4 * i + rows) + q)
        return 0

    lax.fori_loop(0, rows // 2, scatter_far, 0)
    tiles = packed_rows // 2

    def centre(k, _):
        x = jnp.concatenate([window[2 * k], window[2 * k + 1]], axis=1)
        mean = jnp.sum(x, axis=0, keepdims=True) * (1.0 / count)
        x = x - mean
        centred[k] = x
        means[pl.ds(k, 1), :] = mean
        high = x.astype(bf16).astype(f32)
        both = jnp.concatenate([high, x - high], axis=0).T.astype(bf16)
        zero = jnp.zeros((2 * TW, 2 * count), bf16)
        hilo[k, 0, :, 0 : 2 * count] = both
        hilo[k, 0, :, 2 * count : 4 * count] = zero
        hilo[k, 1, :, 0 : 2 * count] = zero
        hilo[k, 1, :, 2 * count : 4 * count] = both
        return 0

    def left(k, base, factor=None):
        x = centred[k]
        mean = means[pl.ds(k, 1), :]
        pieces, vectors = [], []
        for q in range(4):
            w = weight[base + q, pl.ds(k, 1), :]
            u = forced[base + q, pl.ds(k, 1), :]
            if factor is not None:
                w = w * factor
                u = u * factor
            high, low = split(x * w)
            pieces += [high, low]
            vectors.append(u - w * mean)
        v = jnp.concatenate(vectors + [jnp.zeros((4, 2 * TW), f32)], axis=0)
        top = v.astype(bf16).astype(f32)
        pieces.append(jnp.concatenate([top, v - top], axis=0).astype(bf16))
        return jnp.concatenate(pieces, axis=0)

    low_half = lax.broadcasted_iota(i32, (count, TW), 1) < count
    low_row = lax.broadcasted_iota(i32, (1, TW), 1) < count

    def store(ref, at, acc, more=False):
        def put(dst, value):
            ref[dst] = ref[dst] + value if more else value

        folded = []
        for q in range(4):
            x = acc[2 * q * count : (2 * q + 1) * count] + acc[(2 * q + 1) * count : (2 * q + 2) * count]
            folded.append(x + pltpu.roll(x, count, 1))
        v = acc[8 * count : 8 * count + 8] + acc[8 * count + 8 : 8 * count + 16]
        v = v + pltpu.roll(v, count, 1)
        for h in range(2):
            lanes = slice(h * TW, (h + 1) * TW)
            put((at, slice(0, count), lanes), jnp.where(low_half, folded[2 * h], folded[2 * h + 1]))
            row = jnp.where(low_row, v[2 * h : 2 * h + 1], v[2 * h + 1 : 2 * h + 2])
            put((at, slice(count, count + 8), lanes), jnp.broadcast_to(row, (8, TW)))

    main = rows // 2
    part_k = main // 2
    edge_a, edge_b = part_k, 2 * part_k + 1

    def ahead_copy(c):
        return to(c, to_next.at[c], got.at[0, c], nxt, next_send, next_recv)

    def behind_copy(c):
        return to(c, to_prev.at[c + 1], got.at[1, c], prv, prev_send, prev_recv)

    def far(c, _):
        nb = 2 * rows + 4 * c
        pb = 4 * (c - 1)
        acc = None

        def add(acc, k, base, sel, factor=None):
            part = dot_nn(left(k, base, factor), hilo[k, sel])
            return part if acc is None else acc + part

        for k in range(main):
            ahead = 2 * c <= k
            acc = add(acc, k + k // part_k, jnp.where(ahead, nb, pb), jnp.where(ahead, 0, 1))
        ahead = c < 4
        acc = add(acc, edge_b, jnp.where(ahead, nb, pb), jnp.where(ahead, 0, 1))
        behind = c >= 1
        acc = add(acc, edge_a, jnp.where(behind, pb, nb), jnp.where(behind, 1, 0))
        factor = jnp.where((c == 1) | (c == 3), jnp.float32(1.0), jnp.float32(0.0))
        base = jnp.where(c == 1, nb, jnp.where(c == 3, pb, 0))
        acc = add(acc, jnp.where(c == 3, edge_b, edge_a), base, jnp.where(c == 3, 1, 0), factor)
        store(to_next, c, acc[:, 0:TW])
        store(to_prev, c, acc[:, TW : 2 * TW])

        @pl.when(c < 4)
        def _():
            ahead_copy(c).start()

        @pl.when(c >= 1)
        def _():
            behind_copy(c - 1).start()

        return 0

    def near(j, _, part=0):
        acc = None
        for k in range(part * (part_k + 1), (part + 1) * (part_k + 1)):
            piece = dot_nn(left(k, rows + 4 * j), hilo[k, 0, :, 0 : 2 * count])
            acc = piece if acc is None else acc + piece
        store(total, j, acc, part == 1)
        return 0

    for part in range(2):
        own[part].wait()
        for copy in copies[part * (groups - 1) : (part + 1) * (groups - 1)]:
            copy.wait()
        lax.fori_loop(part * (part_k + 1), (part + 1) * (part_k + 1), centre, 0)
        if part == 1:
            lax.fori_loop(0, 5, far, 0)
        lax.fori_loop(0, 4, functools.partial(near, part=part), 0)
    for c in range(4):
        ahead_copy(c).wait()
        behind_copy(c).wait()

    @pl.when(s > 0)
    def _():
        total[...] += got[0]

    @pl.when(s < strips - 1)
    def _():
        total[...] += got[1]


def cycle(members, flow_east, flow_north, mixing, land, lists, counts, cells, values, noises, strips, groups):
    rows, width = members.shape[1:]
    slots = lists.shape[2]
    packed_rows = rows + rows // 4
    tiles = packed_rows // 2
    count = 8 * groups
    tables = [x.reshape(-1, TW) for x in (cells, values, noises)]
    big = [
        pltpu.with_memory_space_constraint(x, pltpu.HBM)
        for x in (members, flow_east, flow_north, mixing, land, lists, counts.reshape(1, rows))
    ]
    tables = [pltpu.with_memory_space_constraint(x, pltpu.HBM) for x in tables]
    dma = pltpu.SemaphoreType.DMA
    far_in = pl.BlockSpec(memory_space=pltpu.HBM)
    return pl.pallas_call(
        functools.partial(cycle_kernel, strips, groups),
        name="cycle",
        out_shape=[
            jax.ShapeDtypeStruct((tiles, count, 2 * TW), f32),
            jax.ShapeDtypeStruct((tiles, 2 * TW), f32),
            jax.ShapeDtypeStruct((4, count + 8, 4 * count), f32),
        ],
        in_specs=[far_in] * 10,
        out_specs=[pl.BlockSpec(memory_space=VMEM)] * 3,
        scratch_shapes=[
            VMEM(members.shape, f32),
            VMEM((rows, width), f32),
            VMEM((rows, width), f32),
            VMEM((rows, width), f32),
            VMEM((rows, width), i32),
            VMEM(lists.shape, i32),
            VMEM((1, rows), i32),
            VMEM(tables[0].shape, i32),
            VMEM(tables[1].shape, f32),
            VMEM(tables[2].shape, f32),
            VMEM((packed_rows, count, TW), f32),
            VMEM((rows + 2 * STEPS, 8, width), f32),
            VMEM((rows + 2 * STEPS, 8, width), f32),
            VMEM((rows + 2 * STEPS, 8, width), f32),
            VMEM((rows + 6, 4, width), f32),
            VMEM((groups, packed_rows, 8, TW), f32),
            VMEM((3 * rows, slots), i32),
            VMEM((3 * rows, slots), i32),
            VMEM((3 * rows, slots), i32),
            VMEM((3 * rows, slots), f32),
            VMEM((3 * rows, slots), f32),
            VMEM((3 * rows, tiles, 2 * TW), f32),
            VMEM((3 * rows, tiles, 2 * TW), f32),
            VMEM((tiles, 2, 2 * TW, 4 * count), bf16),
            VMEM((5, count + 8, 4 * count), f32),
            VMEM((5, count + 8, 4 * count), f32),
            VMEM((2, 4, count + 8, 4 * count), f32),
            dma((10,)), dma((6,)), dma((6,)), dma((2 * (groups - 1),)), dma((2 * (groups - 1),)), dma((2,)),
            dma((4,)), dma((4,)), dma((4,)), dma((4,)),
        ],
        compiler_params=pltpu.CompilerParams(
            collective_id=0, has_side_effects=True, vmem_limit_bytes=40 * 1024 * 1024
        ),
    )(*big, *tables)


def analysis_kernel(gram, centred, means, out, zs, rs, scales):
    quads, count, lanes = zs.shape
    per = lanes // count
    part_k = (centred.shape[0] - 2) // 2
    row_of = lax.broadcasted_iota(i32, (count, lanes), 0)
    lane_of = lax.broadcasted_iota(i32, (count, lanes), 1)
    eye = jnp.where(row_of == lane_of % count, 1.0, 0.0).astype(f32)
    seg_row = lax.broadcasted_iota(i32, (lanes, lanes), 0) // count
    seg_col = lax.broadcasted_iota(i32, (lanes, lanes), 1) // count
    diag = seg_row == seg_col
    diag_one = jnp.where(diag, 1.0, 0.0).astype(bf16)
    every = range(quads)

    def blocked(x):
        return jnp.where(diag, jnp.concatenate([x] * per, axis=0), jnp.zeros((), bf16))

    def right(x):
        return blocked(x[0]), blocked(x[1])

    def mul(a, b):
        (ah, al), (bh, bl) = a, b
        n = ah.shape[0]
        p = dot_nn(jnp.concatenate([ah, al], axis=0), bh)
        return p[:n] + p[n:] + dot_nn(ah, bl)

    b = [eye + gram[g, 0:count, :] / (count - 1) for g in every]
    stacked = []
    for g in every:
        sq = jnp.sum(b[g] * b[g], axis=0, keepdims=True)
        h1 = sq.astype(bf16)
        rest = sq - h1.astype(f32)
        h2 = rest.astype(bf16)
        h3 = (rest - h2.astype(f32)).astype(bf16)
        stacked += [jnp.broadcast_to(h, (16, lanes)) for h in (h1, h2, h3)]
    sums = dot_nn(jnp.concatenate(stacked, axis=0), diag_one)
    z, f = [], []
    for g in every:
        at = 48 * g
        frob = jnp.sqrt(sums[at : at + 1] + sums[at + 16 : at + 17] + sums[at + 32 : at + 33])
        z.append(b[g] / frob)
        scales[pl.ds(g, 1), :] = jnp.sqrt(frob)
        f.append(1.5 * eye - 0.5 * z[g])
        rs[g] = f[g]
    zr = [right(split(z[g])) for g in every]
    for g in every:
        zs[g] = mul(split(f[g]), zr[g])

    def step(i, _):
        r = [split(rs[g]) for g in every]
        z = [split(zs[g]) for g in every]
        zr = [right(z[g]) for g in every]
        f = [right(split(1.5 * eye - 0.5 * mul(r[g], zr[g]))) for g in every]
        for g in every:
            p = dot_nn(jnp.concatenate([z[g][0], z[g][1], r[g][0], r[g][1]], axis=0), f[g][0])
            q = dot_nn(jnp.concatenate([z[g][0], r[g][0]], axis=0), f[g][1])
            zs[g] = p[:count] + p[count : 2 * count] + q[:count]
            rs[g] = p[2 * count : 3 * count] + p[3 * count :] + q[count:]
        return 0

    lax.fori_loop(0, NSITER - 2, step, 0)
    low_half = lax.broadcasted_iota(i32, (count, 2 * count), 1) < count
    r = [split(rs[g]) for g in every]
    zr = [right(split(zs[g])) for g in every]
    f = [right(split(1.5 * eye - 0.5 * mul(r[g], zr[g]))) for g in every]
    t = [mul(r[g], f[g]) / scales[pl.ds(g, 1), :] for g in every]
    tr = [right(split(t[g])) for g in every]
    vec = [jnp.broadcast_to(gram[g, count : count + 1, :], (16, lanes)) for g in every]
    vec = [mul(split(vec[g]), tr[g]) for g in every]
    vec = [mul(split(vec[g]), tr[g]) / (count - 1) for g in every]
    for g in every:
        mix = t[g] + vec[g][0:1]
        for h in range(per // 2):
            two = mix[:, h * 2 * count : (h + 1) * 2 * count]
            pair = g * (per // 2) + h
            k = pair + pair // part_k
            x = split(jnp.concatenate([centred[k, :, 0:TW], centred[k, :, TW : 2 * TW]], axis=0))
            lhs = jnp.concatenate([jnp.where(low_half, two, 0.0), jnp.where(low_half, 0.0, two)], axis=0)
            y = mul(split(lhs), x)
            for q in range(2):
                average = means[k : k + 1, q * TW : (q + 1) * TW]
                out[:, 2 * pair + q, :] = average + y[q * count : (q + 1) * count]


def analyse(gram, centred, means, rows):
    quads, _, lanes = gram.shape
    count = centred.shape[1]
    return pl.pallas_call(
        analysis_kernel,
        name="analysis",
        out_shape=jax.ShapeDtypeStruct((count, rows, TW), f32),
        in_specs=[pl.BlockSpec(memory_space=VMEM)] * 3,
        out_specs=pl.BlockSpec(memory_space=VMEM),
        scratch_shapes=[
            VMEM((quads, count, lanes), f32),
            VMEM((quads, count, lanes), f32),
            VMEM((quads, lanes), f32),
        ],
        compiler_params=pltpu.CompilerParams(vmem_limit_bytes=16 * 1024 * 1024),
    )(gram, centred, means)


def body(strips, groups, members, flow_east, flow_north, mixing, land_mask, sensor_cell,
         sensor_value, sensor_noise, tile_lists, tile_counts):
    centred, means, total = cycle(
        members, flow_east, flow_north, mixing, land_mask, tile_lists, tile_counts,
        sensor_cell, sensor_value, sensor_noise, strips, groups,
    )
    return analyse(total, centred, means, members.shape[1])


def solution(mesh):
    strips, groups = mesh.shape["space"], mesh.shape["mem"]
    in_specs = (
        P("mem", "space", None),
        P("space", None),
        P("space", None),
        P("space", None),
        P("space", None),
        P("space"),
        P("space"),
        P("space"),
        P("space", "mem", None),
        P("space", "mem"),
    )
    return jax.shard_map(
        functools.partial(body, strips, groups),
        mesh=mesh,
        in_specs=in_specs,
        out_specs=P(None, "space", "mem"),
        check_vma=False,
    )
```

```python
import functools

import jax
import jax.numpy as jnp
from jax import lax
from jax.experimental import pallas as pl
from jax.experimental.pallas import tpu as pltpu
from jax.sharding import PartitionSpec as P

TW = 128
STEPS = 4
NSITER = 8
RLOC = 8
EDGE = 16
MESH = pl.DeviceIdType.MESH
VMEM = pltpu.VMEM
f32 = jnp.float32
bf16 = jnp.bfloat16
i32 = jnp.int32


def split(x):
    high = x.astype(bf16)
    return high, (x - high.astype(f32)).astype(bf16)


def dot_nt(a, b):
    return lax.dot_general(a, b, (((1,), (1,)), ((), ())), preferred_element_type=f32)


def dot_nn(a, b):
    return jnp.dot(a, b, preferred_element_type=f32)


def gaspari(ratio):
    capped = jnp.maximum(ratio, 1.0)
    inner = (((-0.25 * ratio + 0.5) * ratio + 0.625) * ratio - 5.0 / 3.0) * ratio * ratio + 1.0
    outer = (
        ((((ratio / 12.0 - 0.5) * ratio + 0.625) * ratio + 5.0 / 3.0) * ratio - 5.0) * ratio
        + 4.0
        - 2.0 / (3.0 * capped)
    )
    return jnp.where(ratio <= 1.0, inner, jnp.where(ratio <= 2.0, outer, 0.0))


def cycle_kernel(
    strips, groups,
    members_h, east_h, north_h, mixing_h, land_h, lists_h, counts_h, cells_h, values_h, noises_h,
    centred, means, total,
    members, flow_east, flow_north, mixing, land, tile_lists, tile_counts, cells, values, noises,
    window, buf0, buf1, buf2, coef, outbox, lists, place_ref, row_ref, w_ref, u_ref,
    weight, forced, hilo, to_next, to_prev, got, next_force, prev_force, got_force,
    load_sem, halo_send, halo_recv, mem_send, mem_recv, own_sem,
    next_send, next_recv, prev_send, prev_recv,
):
    loads = [
        pltpu.make_async_copy(src, dst, load_sem.at[k])
        for k, (src, dst) in enumerate((
            (members_h, members), (land_h, land), (east_h, flow_east), (north_h, flow_north),
            (mixing_h, mixing), (lists_h, tile_lists), (cells_h, cells), (values_h, values),
            (noises_h, noises), (counts_h, tile_counts),
        ))
    ]
    for copy in loads:
        copy.start()
    s = lax.axis_index("space")
    m = lax.axis_index("mem")
    nxt = lax.rem(s + 1, strips)
    prv = lax.rem(s + strips - 1, strips)
    rows = members.shape[1]
    width = members.shape[2]
    slots = tile_lists.shape[2]
    chunks = cells.shape[0]
    per_strip = chunks * TW
    count = 8 * groups
    barrier = pltpu.get_barrier_semaphore()
    for other in (prv, nxt):
        pl.semaphore_signal(barrier, inc=1, device_id={"space": other}, device_id_type=MESH)
    for step in range(1, groups):
        peer = lax.rem(m + step, groups)
        pl.semaphore_signal(barrier, inc=1, device_id={"mem": peer}, device_id_type=MESH)

    def fill(r):
        ocean = land[pl.ds(r, 1), :].astype(f32)
        coef[3 + r, 0:1, :] = 0.5 * flow_east[pl.ds(r, 1), :]
        coef[3 + r, 1:2, :] = 0.5 * flow_north[pl.ds(r, 1), :]
        coef[3 + r, 2:3, :] = mixing[pl.ds(r, 1), :]
        coef[3 + r, 3:4, :] = ocean
        buf0[STEPS + r] = members[:, r, :] * ocean

    for copy in loads:
        copy.wait()
    for r in range(STEPS):
        fill(r)
    for r in range(rows - STEPS, rows):
        fill(r)
    slot = lax.broadcasted_iota(i32, (rows, slots), 1)
    square = lax.broadcasted_iota(i32, (rows, rows), 0) == lax.broadcasted_iota(i32, (rows, rows), 1)
    used = jnp.where(square, jnp.broadcast_to(tile_counts[...].astype(f32), (rows, rows)), 0.0)
    used = jnp.sum(used, axis=1, keepdims=True)
    lists[pl.ds(rows, rows)] = jnp.where(slot.astype(f32) < used, tile_lists[:, 0, :], -(1 << 20))
    pl.semaphore_wait(barrier, 2 + groups - 1)

    def to(k, src, dst, other, send=halo_send, recv=halo_recv):
        return pltpu.make_async_remote_copy(
            src_ref=src, dst_ref=dst, send_sem=send.at[k], recv_sem=recv.at[k],
            device_id={"space": other}, device_id_type=MESH,
        )

    last = STEPS + rows
    mine_l = lists.at[pl.ds(rows, rows)]
    halo = [
        to(0, buf0.at[pl.ds(rows, STEPS)], buf0.at[pl.ds(0, STEPS)], nxt),
        to(1, buf0.at[pl.ds(STEPS, STEPS)], buf0.at[pl.ds(last, STEPS)], prv),
        to(2, coef.at[pl.ds(rows, 3)], coef.at[pl.ds(0, 3)], nxt),
        to(3, coef.at[pl.ds(3, 3)], coef.at[pl.ds(3 + rows, 3)], prv),
        to(4, mine_l, lists.at[pl.ds(0, rows)], nxt),
        to(5, mine_l, lists.at[pl.ds(2 * rows, rows)], prv),
    ]
    for copy in halo:
        copy.start()
    for r in range(STEPS, rows - STEPS):
        fill(r)

    start = m * TW
    middle = start.astype(f32) + (TW - 1) / 2.0
    lane_rows = lax.broadcasted_iota(i32, (8, TW), 0)

    def attributes(d):
        for half in range(rows // 8):
            for side in range(slots // TW):
                at = (pl.ds(pl.multiple_of(rows * d + 8 * half, 8), 8), pl.ds(side * TW, TW))
                j = lists[at] + (d - 2) * per_strip
                usable = (j >= 0) & (j < per_strip)
                j = jnp.where(usable, j, 0)
                low = j & (TW - 1)
                high = j >> 7
                cell = jnp.zeros((8, TW), i32)
                value = jnp.zeros((8, TW), f32)
                noise = jnp.ones((8, TW), f32)
                for c in range(chunks):
                    here = high == c

                    def pick(table, c=c, low=low):
                        full = jnp.broadcast_to(table[c : c + 1, :], (8, TW))
                        return jnp.take_along_axis(full, low, axis=1, mode="promise_in_bounds")

                    cell = jnp.where(here, pick(cells), cell)
                    value = jnp.where(here, pick(values), value)
                    noise = jnp.where(here, pick(noises), noise)
                shift = width.bit_length() - 1
                row = cell >> shift
                col = cell & (width - 1)
                tile_row = lane_rows + (8 * half + (d - 1) * rows)
                dy = (row - tile_row).astype(f32)
                a = jnp.abs(col.astype(f32) - middle)
                a = jnp.minimum(a, float(width) - a)
                dx = jnp.maximum(a - (TW - 1) / 2.0, 0.0)
                distance = jnp.sqrt(dx * dx + dy * dy)
                w = jnp.where(usable, gaspari(distance / RLOC) / noise, 0.0)
                p = (col - start) & (width - 1)
                edge = jnp.where(p < TW + EDGE, p - TW + EDGE, p - (width - EDGE))
                edge = TW + 32 * (row & 3) + edge
                near = (p < TW + EDGE) | (p >= width - EDGE)
                place_ref[at] = jnp.where(p < TW, p, jnp.where(near, edge, -1))
                row_ref[at] = row
                w_ref[at] = w
                u_ref[at] = w * value

    half = rows // 2
    cell_iota = lax.broadcasted_iota(i32, (2 * TW, slots), 0)
    ri = lax.broadcasted_iota(i32, (rows, slots), 0)
    row_iota = 2 * (ri & (half - 1)) + ri // half
    qi = lax.broadcasted_iota(i32, (4, slots), 0)
    quad_iota = 2 * (qi & 1) + (qi >> 1)

    def scatter(t):
        place = place_ref[pl.ds(t, 1), :]
        row = row_ref[pl.ds(t, 1), :]
        hot = jnp.where(cell_iota == place, 1.0, 0.0).astype(bf16)
        parts = []
        for x in (w_ref[pl.ds(t, 1), :], u_ref[pl.ds(t, 1), :]):
            high = x.astype(bf16).astype(f32)
            parts += [high, x - high]
        main = [jnp.where(row_iota == row, x, 0.0) for x in parts]
        quad = [jnp.where(quad_iota == (row >> 2), x, 0.0) for x in parts]
        both = jnp.concatenate(quad, axis=0)
        lhs = jnp.concatenate(main + [both], axis=0).astype(bf16)
        out = dot_nt(lhs, hot)
        for k, ref in ((0, weight), (2, forced)):
            x = out[k * rows : (k + 1) * rows, :TW] + out[(k + 1) * rows : (k + 2) * rows, :TW]
            at = 4 * rows + 4 * k
            e = out[at : at + 4, TW:] + out[at + 4 : at + 8, TW:]
            low, high = x[0:half], x[half:rows]
            part = half // 2
            ref[t, :, 0:TW] = jnp.concatenate([low[:part], e[0:1], low[part:], e[1:2]], axis=0)
            ref[t, :, TW : 2 * TW] = jnp.concatenate([high[:part], e[2:3], high[part:], e[3:4]], axis=0)

    attributes(jnp.int32(1))

    def scatter_own(i, _):
        for q in range(4):
            scatter(rows + 4 * i + q)
        return 0

    lax.fori_loop(0, rows // 4, scatter_own, 0)

    def advance(src, i):
        c = src[i]
        n = src[i + 1]
        so = src[i - 1]
        e = pltpu.roll(c, width - 1, 1)
        w = pltpu.roll(c, 1, 1)
        fe = coef[i - 1, 0:1, :]
        fn = coef[i - 1, 1:2, :]
        mx = coef[i - 1, 2:3, :]
        oc = coef[i - 1, 3:4, :]
        carried = fe * (e - w) + fn * (n - so)
        spread = e + w + n + so - 4.0 * c
        return oc * (c - carried + mx * spread)

    chain = (buf0, buf1, buf2, buf1)
    for step in range(STEPS - 1):
        src, dst = chain[step], chain[step + 1]

        def inner(i, _, src=src, dst=dst, first=STEPS + 1 + step):
            for q in range(2):
                dst[first + 2 * i + q] = advance(src, first + 2 * i + q)
            return 0

        lax.fori_loop(0, (rows - 2 - 2 * step) // 2, inner, 0)

    for copy in halo[:4]:
        copy.wait_recv()

    @pl.when(s == 0)
    def _():
        buf0[pl.ds(0, STEPS)] = jnp.zeros((STEPS, 8, width), f32)
        coef[pl.ds(0, 3)] = jnp.zeros((3, 4, width), f32)

    @pl.when(s == strips - 1)
    def _():
        buf0[pl.ds(last, STEPS)] = jnp.zeros((STEPS, 8, width), f32)
        coef[pl.ds(3 + rows, 3)] = jnp.zeros((3, 4, width), f32)

    for step in range(STEPS - 1):
        src, dst = chain[step], chain[step + 1]

        def outer(i, _, src=src, dst=dst, low=step + 1, high=rows + STEPS - 1 - step):
            dst[low + i] = advance(src, low + i)
            dst[high + i] = advance(src, high + i)
            return 0

        lax.fori_loop(0, STEPS, outer, 0, unroll=2)
    src = chain[STEPS - 1]
    lane = lax.broadcasted_iota(i32, (8, TW), 1)

    packed_rows = window.shape[0]
    chunk = packed_rows // 2

    def final(g, _, shift=0):
        packed = [jnp.zeros((8, TW), f32) for _ in range(groups)]
        for q in range(4):
            r = 4 * g + q
            value = advance(src, STEPS + r)
            blocks = [value[:, b * TW : (b + 1) * TW] for b in range(groups)]
            for b in range(groups):
                outbox[b, r + shift] = blocks[b]
                both = jnp.where(lane < EDGE, blocks[(b + 1) % groups], blocks[(b - 1) % groups])
                turned = pltpu.roll(both, (32 * q + EDGE) % TW, 1)
                packed[b] = jnp.where(lane // 32 == q, turned, packed[b])
        for b in range(groups):
            outbox[b, rows // 2 + 4 * shift + g] = packed[b]
        return 0

    copies, own = [], []
    for part in range(2):
        lax.fori_loop(2 * part, 2 * part + 2, functools.partial(final, shift=2 * part), 0)
        here = pl.ds(chunk * part, chunk)
        mine = window.at[here, pl.ds(pl.multiple_of(8 * m, 8), 8), :]
        for k, step in enumerate((4, 3, 5, 2, 6, 7, 1)):
            peer = lax.rem(m + step, groups)
            at = part * (groups - 1) + k
            copy = pltpu.make_async_remote_copy(
                src_ref=outbox.at[peer, here], dst_ref=mine, send_sem=mem_send.at[at],
                recv_sem=mem_recv.at[at], device_id={"mem": peer}, device_id_type=MESH,
            )
            copy.start()
            copies.append(copy)
        own.append(pltpu.make_async_copy(outbox.at[m, here], mine, own_sem.at[part]))
        own[part].start()

    for copy in halo[4:]:
        copy.wait_recv()

    @pl.when(s == 0)
    def _():
        lists[pl.ds(0, rows)] = jnp.full((rows, slots), -(1 << 20), i32)

    @pl.when(s == strips - 1)
    def _():
        lists[pl.ds(2 * rows, rows)] = jnp.full((rows, slots), -(1 << 20), i32)

    for copy in halo:
        copy.wait_send()

    def attributes_far(i, _):
        attributes(2 * i)
        return 0

    lax.fori_loop(0, 2, attributes_far, 0)

    def scatter_far(i, _):
        for q in range(4):
            scatter(jnp.where(i < rows // 4, 4 * i, 4 * i + rows) + q)
        return 0

    lax.fori_loop(0, rows // 2, scatter_far, 0)
    tiles = packed_rows // 2

    def centre(k, _):
        x = jnp.concatenate([window[2 * k], window[2 * k + 1]], axis=1)
        mean = jnp.sum(x, axis=0, keepdims=True) * (1.0 / count)
        x = x - mean
        centred[k] = x
        means[pl.ds(k, 1), :] = mean
        high = x.astype(bf16).astype(f32)
        both = jnp.concatenate([high, x - high], axis=0).T.astype(bf16)
        hilo[k] = both
        return 0

    def left(k, base):
        x = centred[k]
        mean = means[pl.ds(k, 1), :]
        pieces, vectors = [], []
        for q in range(4):
            w = weight[base + q, pl.ds(k, 1), :]
            pieces += split(x * w)
            vectors.append(forced[base + q, pl.ds(k, 1), :] - w * mean)
        v = jnp.concatenate(vectors + [jnp.zeros((4, 2 * TW), f32)], axis=0)
        top = v.astype(bf16).astype(f32)
        tail = jnp.concatenate([top, v - top], axis=0).astype(bf16)
        return jnp.concatenate(pieces + [tail], axis=0)

    low_half = lax.broadcasted_iota(i32, (count, TW), 1) < count
    low_row = lax.broadcasted_iota(i32, (1, TW), 1) < count
    quarter = count // 2
    upper = (lax.broadcasted_iota(i32, (quarter, TW), 1) & quarter) > 0

    def partial_sums(base, need):
        acc = None
        for k in need:
            part = dot_nn(left(k, base), hilo[k])
            acc = part if acc is None else acc + part
        folded = []
        for q in range(4):
            x = acc[2 * q * count : (2 * q + 1) * count] + acc[(2 * q + 1) * count : (2 * q + 2) * count]
            folded.append(x + pltpu.roll(x, count, 1))
        v = acc[8 * count : 8 * count + 8] + acc[8 * count + 8 : 8 * count + 16]
        v = v + pltpu.roll(v, count, 1)
        squares, rows_of = [], []
        for h in range(2):
            squares.append(jnp.where(low_half, folded[2 * h], folded[2 * h + 1]))
            rows_of.append(jnp.where(low_row, v[2 * h : 2 * h + 1], v[2 * h + 1 : 2 * h + 2]))
        return squares, rows_of

    main = rows // 2
    part_k = main // 2
    edge_a, edge_b = part_k, 2 * part_k + 1

    def near(j, _, part=0):
        squares, rows_of = partial_sums(
            rows + 4 * j, range(part * (part_k + 1), (part + 1) * (part_k + 1))
        )
        for h in range(2):
            lanes = slice(h * TW, (h + 1) * TW)
            wide = jnp.broadcast_to(rows_of[h], (8, TW))
            if part == 0:
                total[j, 0:count, lanes] = squares[h]
                total[j, count : count + 8, lanes] = wide
            else:
                total[j, 0:count, lanes] += squares[h]
                total[j, count : count + 8, lanes] += wide
        return 0

    def far(c, base, need, out, out_force):
        squares, rows_of = partial_sums(base, need)
        for h in range(2):
            lanes = slice(h * TW, (h + 1) * TW)
            out[c, 0:quarter, lanes] = squares[h][0:quarter]
            out_force[c : c + 1, lanes] = rows_of[h]
        last_part = jnp.where(upper, squares[0][quarter:], pltpu.roll(squares[1][quarter:], TW - quarter, 1))
        out[c, quarter : quarter + quarter // 2, 0:TW] = last_part[: quarter // 2]
        out[c, quarter : quarter + quarter // 2, TW : 2 * TW] = last_part[quarter // 2 :]

    def ahead_copy(c):
        return to(c, to_next.at[c], got.at[0, c], nxt, next_send, next_recv)

    def behind_copy(c):
        return to(c, to_prev.at[c], got.at[1, c], prv, prev_send, prev_recv)

    ahead_force = to(4, next_force, got_force.at[0], nxt, next_send, next_recv)
    behind_force = to(4, prev_force, got_force.at[1], prv, prev_send, prev_recv)
    next_force[...] = jnp.zeros(next_force.shape, f32)
    prev_force[...] = jnp.zeros(prev_force.shape, f32)

    def at_k(k):
        return k + k // part_k

    def ahead(c):
        need = [at_k(k) for k in range(2 * c, main)]
        need += [edge_a, edge_b] if c < 2 else [edge_b]
        far(c, 2 * rows + 4 * c, need, to_next, next_force)

    def behind(c):
        need = [at_k(k) for k in range(0, 2 * c + 2)]
        need += [edge_a] if c < 2 else [edge_a, edge_b]
        far(c, 4 * c, need, to_prev, prev_force)

    for part in range(2):
        own[part].wait()
        for copy in copies[part * (groups - 1) : (part + 1) * (groups - 1)]:
            copy.wait()
        first = part * (part_k + 1)
        lax.fori_loop(first, first + part_k + 1, centre, 0, unroll=part_k + 1)
        if part == 0:
            behind(0)
            behind(1)
            behind_copy(0).start()
            behind_copy(1).start()
        else:
            ahead(3)
            ahead(2)
            ahead_copy(3).start()
            ahead_copy(2).start()
            ahead(1)
            behind(2)
            ahead_copy(1).start()
            behind_copy(2).start()
            ahead(0)
            behind(3)
            ahead_copy(0).start()
            ahead_force.start()
            behind_copy(3).start()
            behind_force.start()
        lax.fori_loop(0, 4, functools.partial(near, part=part), 0, unroll=2)
    for c in range(4):
        ahead_copy(c).wait()
        behind_copy(c).wait()
    ahead_force.wait()
    behind_force.wait()

    def both(ref, at):
        return jnp.where(s > 0, ref[(0, *at)], 0.0) + jnp.where(s < strips - 1, ref[(1, *at)], 0.0)

    more = both(got_force, (slice(0, 8), slice(0, 2 * TW)))
    blank = jnp.zeros((quarter, TW), f32)
    for g in range(4):
        extra = both(got, (g,))
        packed = jnp.concatenate(
            [extra[quarter : quarter + quarter // 2, 0:TW], extra[quarter : quarter + quarter // 2, TW:]], axis=0
        )
        for h in range(2):
            lanes = slice(h * TW, (h + 1) * TW)
            top = extra[0:quarter, lanes]
            turned = jnp.concatenate(
                [pltpu.roll(top, TW - quarter, 1), blank, pltpu.roll(top, quarter, 1), blank], axis=0
            ).T[0:quarter]
            corner = packed if h == 0 else pltpu.roll(packed, quarter, 1)
            total[g, 0:quarter, lanes] += top
            total[g, quarter:count, lanes] += jnp.where(upper, corner, turned)
            total[g, count : count + 8, lanes] += jnp.broadcast_to(more[g : g + 1, lanes], (8, TW))


def cycle(members, flow_east, flow_north, mixing, land, lists, counts, cells, values, noises, strips, groups):
    rows, width = members.shape[1:]
    slots = lists.shape[2]
    packed_rows = rows + rows // 4
    tiles = packed_rows // 2
    count = 8 * groups
    tables = [x.reshape(-1, TW) for x in (cells, values, noises)]
    big = [
        pltpu.with_memory_space_constraint(x, pltpu.HBM)
        for x in (members, flow_east, flow_north, mixing, land, lists, counts.reshape(1, rows))
    ]
    tables = [pltpu.with_memory_space_constraint(x, pltpu.HBM) for x in tables]
    dma = pltpu.SemaphoreType.DMA
    far_in = pl.BlockSpec(memory_space=pltpu.HBM)
    return pl.pallas_call(
        functools.partial(cycle_kernel, strips, groups),
        name="cycle",
        out_shape=[
            jax.ShapeDtypeStruct((tiles, count, 2 * TW), f32),
            jax.ShapeDtypeStruct((tiles, 2 * TW), f32),
            jax.ShapeDtypeStruct((4, count + 8, 4 * count), f32),
        ],
        in_specs=[far_in] * 10,
        out_specs=[pl.BlockSpec(memory_space=VMEM)] * 3,
        scratch_shapes=[
            VMEM(members.shape, f32),
            VMEM((rows, width), f32),
            VMEM((rows, width), f32),
            VMEM((rows, width), f32),
            VMEM((rows, width), i32),
            VMEM(lists.shape, i32),
            VMEM((1, rows), i32),
            VMEM(tables[0].shape, i32),
            VMEM(tables[1].shape, f32),
            VMEM(tables[2].shape, f32),
            VMEM((packed_rows, count, TW), f32),
            VMEM((rows + 2 * STEPS, 8, width), f32),
            VMEM((rows + 2 * STEPS, 8, width), f32),
            VMEM((rows + 2 * STEPS, 8, width), f32),
            VMEM((rows + 6, 4, width), f32),
            VMEM((groups, packed_rows, 8, TW), f32),
            VMEM((3 * rows, slots), i32),
            VMEM((3 * rows, slots), i32),
            VMEM((3 * rows, slots), i32),
            VMEM((3 * rows, slots), f32),
            VMEM((3 * rows, slots), f32),
            VMEM((3 * rows, tiles, 2 * TW), f32),
            VMEM((3 * rows, tiles, 2 * TW), f32),
            VMEM((tiles, 2 * TW, 2 * count), bf16),
            VMEM((4, 3 * count // 4, 4 * count), f32),
            VMEM((4, 3 * count // 4, 4 * count), f32),
            VMEM((2, 4, 3 * count // 4, 4 * count), f32),
            VMEM((8, 4 * count), f32),
            VMEM((8, 4 * count), f32),
            VMEM((2, 8, 4 * count), f32),
            dma((10,)), dma((6,)), dma((6,)), dma((2 * (groups - 1),)), dma((2 * (groups - 1),)), dma((2,)),
            dma((5,)), dma((5,)), dma((5,)), dma((5,)),
        ],
        compiler_params=pltpu.CompilerParams(
            collective_id=0, has_side_effects=True, vmem_limit_bytes=40 * 1024 * 1024
        ),
    )(*big, *tables)


def analysis_kernel(gram, centred, means, out, zs, rs, scales):
    quads, count, lanes = zs.shape
    per = lanes // count
    part_k = (centred.shape[0] - 2) // 2
    row_of = lax.broadcasted_iota(i32, (count, lanes), 0)
    lane_of = lax.broadcasted_iota(i32, (count, lanes), 1)
    eye = jnp.where(row_of == lane_of % count, 1.0, 0.0).astype(f32)
    seg_row = lax.broadcasted_iota(i32, (lanes, lanes), 0) // count
    seg_col = lax.broadcasted_iota(i32, (lanes, lanes), 1) // count
    diag = seg_row == seg_col
    diag_one = jnp.where(diag, 1.0, 0.0).astype(bf16)
    every = range(quads)

    def blocked(x):
        return jnp.where(diag, jnp.concatenate([x] * per, axis=0), jnp.zeros((), bf16))

    def right(x):
        return blocked(x[0]), blocked(x[1])

    def mul(a, b):
        (ah, al), (bh, bl) = a, b
        n = ah.shape[0]
        p = dot_nn(jnp.concatenate([ah, al], axis=0), bh)
        return p[:n] + p[n:] + dot_nn(ah, bl)

    b = [eye + gram[g, 0:count, :] / (count - 1) for g in every]
    stacked = []
    for g in every:
        sq = jnp.sum(b[g] * b[g], axis=0, keepdims=True)
        h1 = sq.astype(bf16)
        rest = sq - h1.astype(f32)
        h2 = rest.astype(bf16)
        h3 = (rest - h2.astype(f32)).astype(bf16)
        stacked += [jnp.broadcast_to(h, (16, lanes)) for h in (h1, h2, h3)]
    sums = dot_nn(jnp.concatenate(stacked, axis=0), diag_one)
    z, f = [], []
    for g in every:
        at = 48 * g
        frob = jnp.sqrt(sums[at : at + 1] + sums[at + 16 : at + 17] + sums[at + 32 : at + 33])
        z.append(b[g] / frob)
        scales[pl.ds(g, 1), :] = jnp.sqrt(frob)
        f.append(1.5 * eye - 0.5 * z[g])
        rs[g] = f[g]
    zr = [right(split(z[g])) for g in every]
    for g in every:
        zs[g] = mul(split(f[g]), zr[g])

    def step(i, _):
        r = [split(rs[g]) for g in every]
        z = [split(zs[g]) for g in every]
        zr = [right(z[g]) for g in every]
        f = [right(split(1.5 * eye - 0.5 * mul(r[g], zr[g]))) for g in every]
        for g in every:
            p = dot_nn(jnp.concatenate([z[g][0], z[g][1], r[g][0], r[g][1]], axis=0), f[g][0])
            q = dot_nn(jnp.concatenate([z[g][0], r[g][0]], axis=0), f[g][1])
            zs[g] = p[:count] + p[count : 2 * count] + q[:count]
            rs[g] = p[2 * count : 3 * count] + p[3 * count :] + q[count:]
        return 0

    lax.fori_loop(0, NSITER - 2, step, 0, unroll=3)
    low_half = lax.broadcasted_iota(i32, (count, 2 * count), 1) < count
    r = [split(rs[g]) for g in every]
    zr = [right(split(zs[g])) for g in every]
    f = [right(split(1.5 * eye - 0.5 * mul(r[g], zr[g]))) for g in every]
    t = [mul(r[g], f[g]) / scales[pl.ds(g, 1), :] for g in every]
    tr = [right(split(t[g])) for g in every]
    vec = [jnp.broadcast_to(gram[g, count : count + 1, :], (16, lanes)) for g in every]
    vec = [mul(split(vec[g]), tr[g]) for g in every]
    vec = [mul(split(vec[g]), tr[g]) / (count - 1) for g in every]
    for g in every:
        mix = t[g] + vec[g][0:1]
        for h in range(per // 2):
            two = mix[:, h * 2 * count : (h + 1) * 2 * count]
            pair = g * (per // 2) + h
            k = pair + pair // part_k
            x = split(jnp.concatenate([centred[k, :, 0:TW], centred[k, :, TW : 2 * TW]], axis=0))
            lhs = jnp.concatenate([jnp.where(low_half, two, 0.0), jnp.where(low_half, 0.0, two)], axis=0)
            y = mul(split(lhs), x)
            for q in range(2):
                average = means[k : k + 1, q * TW : (q + 1) * TW]
                out[:, 2 * pair + q, :] = average + y[q * count : (q + 1) * count]


def analyse(gram, centred, means, rows):
    quads, _, lanes = gram.shape
    count = centred.shape[1]
    return pl.pallas_call(
        analysis_kernel,
        name="analysis",
        out_shape=jax.ShapeDtypeStruct((count, rows, TW), f32),
        in_specs=[pl.BlockSpec(memory_space=VMEM)] * 3,
        out_specs=pl.BlockSpec(memory_space=VMEM),
        scratch_shapes=[
            VMEM((quads, count, lanes), f32),
            VMEM((quads, count, lanes), f32),
            VMEM((quads, lanes), f32),
        ],
        compiler_params=pltpu.CompilerParams(vmem_limit_bytes=16 * 1024 * 1024),
    )(gram, centred, means)


def body(strips, groups, members, flow_east, flow_north, mixing, land_mask, sensor_cell,
         sensor_value, sensor_noise, tile_lists, tile_counts):
    centred, means, total = cycle(
        members, flow_east, flow_north, mixing, land_mask, tile_lists, tile_counts,
        sensor_cell, sensor_value, sensor_noise, strips, groups,
    )
    return analyse(total, centred, means, members.shape[1])


def solution(mesh):
    strips, groups = mesh.shape["space"], mesh.shape["mem"]
    in_specs = (
        P("mem", "space", None),
        P("space", None),
        P("space", None),
        P("space", None),
        P("space", None),
        P("space"),
        P("space"),
        P("space"),
        P("space", "mem", None),
        P("space", "mem"),
    )
    return jax.shard_map(
        functools.partial(body, strips, groups),
        mesh=mesh,
        in_specs=in_specs,
        out_specs=P(None, "space", "mem"),
        check_vma=False,
    )
```

```python
import functools

import jax
import jax.numpy as jnp
from jax import lax
from jax.experimental import pallas as pl
from jax.experimental.pallas import tpu as pltpu
from jax.sharding import PartitionSpec as P

TW = 128
STEPS = 4
NSITER = 8
RLOC = 8
EDGE = 16
PAIR_AT = (5, 6, 0, 1, 2, 3, 7, 8)
MESH = pl.DeviceIdType.MESH
VMEM = pltpu.VMEM
f32 = jnp.float32
bf16 = jnp.bfloat16
i32 = jnp.int32


def split(x):
    high = x.astype(bf16)
    return high, (x - high.astype(f32)).astype(bf16)


def dot_nt(a, b):
    return lax.dot_general(a, b, (((1,), (1,)), ((), ())), preferred_element_type=f32)


def dot_nn(a, b):
    return jnp.dot(a, b, preferred_element_type=f32)


def gaspari(ratio):
    capped = jnp.maximum(ratio, 1.0)
    inner = (((-0.25 * ratio + 0.5) * ratio + 0.625) * ratio - 5.0 / 3.0) * ratio * ratio + 1.0
    outer = (
        ((((ratio / 12.0 - 0.5) * ratio + 0.625) * ratio + 5.0 / 3.0) * ratio - 5.0) * ratio
        + 4.0
        - 2.0 / (3.0 * capped)
    )
    return jnp.where(ratio <= 1.0, inner, jnp.where(ratio <= 2.0, outer, 0.0))


def cycle_kernel(
    strips, groups,
    members_h, east_h, north_h, mixing_h, land_h, lists_h, counts_h, cells_h, values_h, noises_h,
    centred, means, total,
    members, flow_east, flow_north, mixing, land, tile_lists, tile_counts, cells, values, noises,
    window, buf0, buf1, buf2, coef, outbox, lists, place_ref, row_ref, w_ref, u_ref,
    weight, forced, hilo, to_next, to_prev, got, next_force, prev_force, got_force,
    load_sem, halo_send, halo_recv, mem_send, mem_recv, own_sem,
    next_send, next_recv, prev_send, prev_recv,
):
    loads = [
        pltpu.make_async_copy(src, dst, load_sem.at[k])
        for k, (src, dst) in enumerate((
            (members_h, members), (land_h, land), (east_h, flow_east), (north_h, flow_north),
            (mixing_h, mixing), (lists_h, tile_lists), (cells_h, cells), (values_h, values),
            (noises_h, noises), (counts_h, tile_counts),
        ))
    ]
    for copy in loads:
        copy.start()
    s = lax.axis_index("space")
    m = lax.axis_index("mem")
    nxt = lax.rem(s + 1, strips)
    prv = lax.rem(s + strips - 1, strips)
    rows = members.shape[1]
    width = members.shape[2]
    slots = tile_lists.shape[2]
    chunks = cells.shape[0]
    per_strip = chunks * TW
    count = 8 * groups
    barrier = pltpu.get_barrier_semaphore()
    has_prev, has_next = s > 0, s < strips - 1

    def when(wanted, actions):
        @pl.when(wanted)
        def _():
            for action in actions:
                action()

    def greet(other):
        pl.semaphore_signal(barrier, inc=1, device_id={"space": other}, device_id_type=MESH)

    when(has_prev, [lambda: greet(prv)])
    when(has_next, [lambda: greet(nxt)])
    for step in range(1, groups):
        peer = lax.rem(m + step, groups)
        pl.semaphore_signal(barrier, inc=1, device_id={"mem": peer}, device_id_type=MESH)

    def fill(r):
        ocean = land[pl.ds(r, 1), :].astype(f32)
        coef[3 + r, 0:1, :] = 0.5 * flow_east[pl.ds(r, 1), :]
        coef[3 + r, 1:2, :] = 0.5 * flow_north[pl.ds(r, 1), :]
        coef[3 + r, 2:3, :] = mixing[pl.ds(r, 1), :]
        coef[3 + r, 3:4, :] = ocean
        buf0[STEPS + r] = members[:, r, :] * ocean

    for copy in loads:
        copy.wait()
    for r in range(STEPS):
        fill(r)
    for r in range(rows - STEPS, rows):
        fill(r)
    slot = lax.broadcasted_iota(i32, (rows, slots), 1)
    square = lax.broadcasted_iota(i32, (rows, rows), 0) == lax.broadcasted_iota(i32, (rows, rows), 1)
    used = jnp.where(square, jnp.broadcast_to(tile_counts[...].astype(f32), (rows, rows)), 0.0)
    used = jnp.sum(used, axis=1, keepdims=True)
    lists[pl.ds(rows, rows)] = jnp.where(slot.astype(f32) < used, tile_lists[:, 0, :], -(1 << 20))
    pl.semaphore_wait(barrier, groups - 1 + has_prev.astype(i32) + has_next.astype(i32))

    def to(k, src, dst, other, send=halo_send, recv=halo_recv):
        return pltpu.make_async_remote_copy(
            src_ref=src, dst_ref=dst, send_sem=send.at[k], recv_sem=recv.at[k],
            device_id={"space": other}, device_id_type=MESH,
        )

    last = STEPS + rows
    mine_l = lists.at[pl.ds(rows, rows)]
    halo = [
        to(0, buf0.at[pl.ds(rows, STEPS)], buf0.at[pl.ds(0, STEPS)], nxt),
        to(1, buf0.at[pl.ds(STEPS, STEPS)], buf0.at[pl.ds(last, STEPS)], prv),
        to(2, coef.at[pl.ds(rows, 3)], coef.at[pl.ds(0, 3)], nxt),
        to(3, coef.at[pl.ds(3, 3)], coef.at[pl.ds(3 + rows, 3)], prv),
        to(4, mine_l, lists.at[pl.ds(0, rows)], nxt),
        to(5, mine_l, lists.at[pl.ds(2 * rows, rows)], prv),
    ]
    ahead_halo, behind_halo = halo[0::2], halo[1::2]
    when(has_next, [copy.start for copy in ahead_halo])
    when(has_prev, [copy.start for copy in behind_halo])
    for r in range(STEPS, rows - STEPS):
        fill(r)

    start = m * TW
    middle = start.astype(f32) + (TW - 1) / 2.0
    lane_rows = lax.broadcasted_iota(i32, (8, TW), 0)

    def attributes(d):
        for half in range(rows // 8):
            for side in range(slots // TW):
                at = (pl.ds(pl.multiple_of(rows * d + 8 * half, 8), 8), pl.ds(side * TW, TW))
                j = lists[at] + (d - 2) * per_strip
                usable = (j >= 0) & (j < per_strip)
                j = jnp.where(usable, j, 0)
                low = j & (TW - 1)
                high = j >> 7
                cell = jnp.zeros((8, TW), i32)
                value = jnp.zeros((8, TW), f32)
                noise = jnp.ones((8, TW), f32)
                for c in range(chunks):
                    here = high == c

                    def pick(table, c=c, low=low):
                        full = jnp.broadcast_to(table[c : c + 1, :], (8, TW))
                        return jnp.take_along_axis(full, low, axis=1, mode="promise_in_bounds")

                    cell = jnp.where(here, pick(cells), cell)
                    value = jnp.where(here, pick(values), value)
                    noise = jnp.where(here, pick(noises), noise)
                shift = width.bit_length() - 1
                row = cell >> shift
                col = cell & (width - 1)
                tile_row = lane_rows + (8 * half + (d - 1) * rows)
                dy = (row - tile_row).astype(f32)
                a = jnp.abs(col.astype(f32) - middle)
                a = jnp.minimum(a, float(width) - a)
                dx = jnp.maximum(a - (TW - 1) / 2.0, 0.0)
                distance = jnp.sqrt(dx * dx + dy * dy)
                w = jnp.where(usable, gaspari(distance / RLOC) / noise, 0.0)
                p = (col - start) & (width - 1)
                edge = jnp.where(p < TW + EDGE, p - TW + EDGE, p - (width - EDGE))
                edge = TW + 32 * (row & 3) + edge
                near = (p < TW + EDGE) | (p >= width - EDGE)
                place_ref[at] = jnp.where(p < TW, p, jnp.where(near, edge, -1))
                row_ref[at] = row
                w_ref[at] = w
                u_ref[at] = w * value

    half = rows // 2
    cell_iota = lax.broadcasted_iota(i32, (2 * TW, slots), 0)
    ri = lax.broadcasted_iota(i32, (rows, slots), 0)
    row_iota = 2 * (ri & (half - 1)) + ri // half
    qi = lax.broadcasted_iota(i32, (4, slots), 0)
    quad_iota = 2 * (qi & 1) + (qi >> 1)

    def scatter(t):
        place = place_ref[pl.ds(t, 1), :]
        row = row_ref[pl.ds(t, 1), :]
        hot = jnp.where(cell_iota == place, 1.0, 0.0).astype(bf16)
        parts = []
        for x in (w_ref[pl.ds(t, 1), :], u_ref[pl.ds(t, 1), :]):
            high = x.astype(bf16).astype(f32)
            parts += [high, x - high]
        main = [jnp.where(row_iota == row, x, 0.0) for x in parts]
        quad = [jnp.where(quad_iota == (row >> 2), x, 0.0) for x in parts]
        both = jnp.concatenate(quad, axis=0)
        lhs = jnp.concatenate(main + [both], axis=0).astype(bf16)
        out = dot_nt(lhs, hot)
        for k, ref in ((0, weight), (2, forced)):
            x = out[k * rows : (k + 1) * rows, :TW] + out[(k + 1) * rows : (k + 2) * rows, :TW]
            at = 4 * rows + 4 * k
            e = out[at : at + 4, TW:] + out[at + 4 : at + 8, TW:]
            low, high = x[0:half], x[half:rows]
            ref[t, :, 0:TW] = jnp.concatenate([low[2:6], e[2:3], low[0:2], low[6:8], e[0:1]], axis=0)
            ref[t, :, TW : 2 * TW] = jnp.concatenate(
                [high[2:6], e[1:2], high[0:2], high[6:8], e[3:4]], axis=0
            )

    def advance(src, i):
        c = src[i]
        n = src[i + 1]
        so = src[i - 1]
        e = pltpu.roll(c, width - 1, 1)
        w = pltpu.roll(c, 1, 1)
        fe = coef[i - 1, 0:1, :]
        fn = coef[i - 1, 1:2, :]
        mx = coef[i - 1, 2:3, :]
        oc = coef[i - 1, 3:4, :]
        carried = fe * (e - w) + fn * (n - so)
        spread = e + w + n + so - 4.0 * c
        return oc * (c - carried + mx * spread)

    chain = (buf0, buf1, buf2, buf1)
    for step in range(STEPS - 1):
        src, dst = chain[step], chain[step + 1]

        def inner(i, _, src=src, dst=dst, first=STEPS + 1 + step):
            for q in range(2):
                dst[first + 2 * i + q] = advance(src, first + 2 * i + q)
            return 0

        lax.fori_loop(0, (rows - 2 - 2 * step) // 2, inner, 0)

    lane = lax.broadcasted_iota(i32, (8, TW), 1)

    packed_rows = window.shape[0]
    chunk = packed_rows // 2

    def final(i, _, part=0):
        g, base, edges = ((1 + i, 4 * i, 8 + i), (3 * i, 10 + 4 * i, 18 + i))[part]
        packed = [jnp.zeros((8, TW), f32) for _ in range(groups)]
        for q in range(4):
            value = advance(chain[STEPS - 1], STEPS + 4 * g + q)
            blocks = [value[:, b * TW : (b + 1) * TW] for b in range(groups)]
            for b in range(groups):
                outbox[b, base + q] = blocks[b]
                both = jnp.where(lane < EDGE, blocks[(b + 1) % groups], blocks[(b - 1) % groups])
                turned = pltpu.roll(both, (32 * q + EDGE) % TW, 1)
                packed[b] = jnp.where(lane // 32 == q, turned, packed[b])
        for b in range(groups):
            outbox[b, edges] = packed[b]
        return 0

    copies, own = [], []

    def exchange(part):
        lax.fori_loop(0, 2, functools.partial(final, part=part), 0)
        here = pl.ds(chunk * part, chunk)
        mine = window.at[here, pl.ds(pl.multiple_of(8 * m, 8), 8), :]
        for k, step in enumerate((4, 3, 5, 2, 6, 7, 1)):
            peer = lax.rem(m + step, groups)
            at = part * (groups - 1) + k
            copy = pltpu.make_async_remote_copy(
                src_ref=outbox.at[peer, here], dst_ref=mine, send_sem=mem_send.at[at],
                recv_sem=mem_recv.at[at], device_id={"mem": peer}, device_id_type=MESH,
            )
            copy.start()
            copies.append(copy)
        own.append(pltpu.make_async_copy(outbox.at[m, here], mine, own_sem.at[part]))
        own[part].start()

    exchange(0)
    attributes(jnp.int32(1))

    def scatter_own(i, _):
        for q in range(4):
            scatter(rows + 4 * i + q)
        return 0

    lax.fori_loop(0, rows // 4, scatter_own, 0)

    when(has_prev, [copy.wait_recv for copy in ahead_halo[:2]])
    when(has_next, [copy.wait_recv for copy in behind_halo[:2]])

    @pl.when(s == 0)
    def _():
        buf0[pl.ds(0, STEPS)] = jnp.zeros((STEPS, 8, width), f32)
        coef[pl.ds(0, 3)] = jnp.zeros((3, 4, width), f32)

    @pl.when(s == strips - 1)
    def _():
        buf0[pl.ds(last, STEPS)] = jnp.zeros((STEPS, 8, width), f32)
        coef[pl.ds(3 + rows, 3)] = jnp.zeros((3, 4, width), f32)

    for step in range(STEPS - 1):
        src, dst = chain[step], chain[step + 1]

        def outer(i, _, src=src, dst=dst, low=step + 1, high=rows + STEPS - 1 - step):
            dst[low + i] = advance(src, low + i)
            dst[high + i] = advance(src, high + i)
            return 0

        lax.fori_loop(0, STEPS, outer, 0, unroll=2)
    exchange(1)
    when(has_prev, [ahead_halo[2].wait_recv])
    when(has_next, [behind_halo[2].wait_recv])

    @pl.when(s == 0)
    def _():
        lists[pl.ds(0, rows)] = jnp.full((rows, slots), -(1 << 20), i32)

    @pl.when(s == strips - 1)
    def _():
        lists[pl.ds(2 * rows, rows)] = jnp.full((rows, slots), -(1 << 20), i32)

    when(has_next, [copy.wait_send for copy in ahead_halo])
    when(has_prev, [copy.wait_send for copy in behind_halo])

    def attributes_far(i, _):
        attributes(2 * i)
        return 0

    lax.fori_loop(0, 2, attributes_far, 0)

    def scatter_far(i, _):
        for q in range(4):
            scatter(jnp.where(i < rows // 4, 4 * i, 4 * i + rows) + q)
        return 0

    lax.fori_loop(0, rows // 2, scatter_far, 0)
    tiles = packed_rows // 2

    def centre(k, _):
        x = jnp.concatenate([window[2 * k], window[2 * k + 1]], axis=1)
        mean = jnp.sum(x, axis=0, keepdims=True) * (1.0 / count)
        x = x - mean
        centred[k] = x
        means[pl.ds(k, 1), :] = mean
        high = x.astype(bf16).astype(f32)
        both = jnp.concatenate([high, x - high], axis=0).T.astype(bf16)
        hilo[k] = both
        return 0

    def left(k, base):
        x = centred[k]
        mean = means[pl.ds(k, 1), :]
        pieces, vectors = [], []
        for q in range(4):
            w = weight[base + q, pl.ds(k, 1), :]
            pieces += split(x * w)
            vectors.append(forced[base + q, pl.ds(k, 1), :] - w * mean)
        v = jnp.concatenate(vectors + [jnp.zeros((4, 2 * TW), f32)], axis=0)
        top = v.astype(bf16).astype(f32)
        tail = jnp.concatenate([top, v - top], axis=0).astype(bf16)
        return jnp.concatenate(pieces + [tail], axis=0)

    low_half = lax.broadcasted_iota(i32, (count, TW), 1) < count
    low_row = lax.broadcasted_iota(i32, (1, TW), 1) < count
    quarter = count // 2
    upper = (lax.broadcasted_iota(i32, (quarter, TW), 1) & quarter) > 0

    def partial_sums(base, need):
        acc = None
        for k in need:
            part = dot_nn(left(k, base), hilo[k])
            acc = part if acc is None else acc + part
        folded = []
        for q in range(4):
            x = acc[2 * q * count : (2 * q + 1) * count] + acc[(2 * q + 1) * count : (2 * q + 2) * count]
            folded.append(x + pltpu.roll(x, count, 1))
        v = acc[8 * count : 8 * count + 8] + acc[8 * count + 8 : 8 * count + 16]
        v = v + pltpu.roll(v, count, 1)
        squares, rows_of = [], []
        for h in range(2):
            squares.append(jnp.where(low_half, folded[2 * h], folded[2 * h + 1]))
            rows_of.append(jnp.where(low_row, v[2 * h : 2 * h + 1], v[2 * h + 1 : 2 * h + 2]))
        return squares, rows_of

    main = rows // 2
    part_k = main // 2
    edge_a, edge_b = part_k, 2 * part_k + 1

    def near(j, _, part=0):
        squares, rows_of = partial_sums(
            rows + 4 * j, range(part * (part_k + 1), (part + 1) * (part_k + 1))
        )
        for h in range(2):
            lanes = slice(h * TW, (h + 1) * TW)
            wide = jnp.broadcast_to(rows_of[h], (8, TW))
            if part == 0:
                total[j, 0:count, lanes] = squares[h]
                total[j, count : count + 8, lanes] = wide
            else:
                total[j, 0:count, lanes] += squares[h]
                total[j, count : count + 8, lanes] += wide
        return 0

    def far(c, base, need, out, out_force):
        squares, rows_of = partial_sums(base, need)
        for h in range(2):
            lanes = slice(h * TW, (h + 1) * TW)
            out[c, 0:quarter, lanes] = squares[h][0:quarter]
            out_force[c : c + 1, lanes] = rows_of[h]
        last_part = jnp.where(upper, squares[0][quarter:], pltpu.roll(squares[1][quarter:], TW - quarter, 1))
        out[c, quarter : quarter + quarter // 2, 0:TW] = last_part[: quarter // 2]
        out[c, quarter : quarter + quarter // 2, TW : 2 * TW] = last_part[quarter // 2 :]

    def ahead_copy(c):
        return to(c, to_next.at[c], got.at[0, c], nxt, next_send, next_recv)

    def behind_copy(c):
        return to(c, to_prev.at[c], got.at[1, c], prv, prev_send, prev_recv)

    ahead_force = to(4, next_force, got_force.at[0], nxt, next_send, next_recv)
    behind_force = to(4, prev_force, got_force.at[1], prv, prev_send, prev_recv)
    for side, absent in enumerate((s == 0, s == strips - 1)):

        @pl.when(absent)
        def _(side=side):
            got[side] = jnp.zeros(got.shape[1:], f32)
            got_force[side] = jnp.zeros(got_force.shape[1:], f32)

    next_force[...] = jnp.zeros(next_force.shape, f32)
    prev_force[...] = jnp.zeros(prev_force.shape, f32)

    def ahead(c):
        need = [PAIR_AT[p] for p in range(2 * c, main)]
        need += [edge_a, edge_b] if c < 3 else [edge_b]
        far(c, 2 * rows + 4 * c, need, to_next, next_force)

    def behind(c):
        need = [PAIR_AT[p] for p in range(0, 2 * c + 2)]
        need += [edge_b] if c == 0 else [edge_a, edge_b]
        far(c, 4 * c, need, to_prev, prev_force)

    for part in range(2):
        own[part].wait()
        for copy in copies[part * (groups - 1) : (part + 1) * (groups - 1)]:
            copy.wait()
        first = part * (part_k + 1)
        lax.fori_loop(first, first + part_k + 1, centre, 0, unroll=part_k + 1)
        if part == 1:
            for c in range(4):
                ahead(3 - c)
                behind(c)
                when(has_next, [ahead_copy(3 - c).start] + ([ahead_force.start] if c == 3 else []))
                when(has_prev, [behind_copy(c).start] + ([behind_force.start] if c == 3 else []))
        lax.fori_loop(0, 4, functools.partial(near, part=part), 0, unroll=2)
    ahead_all = [ahead_copy(c) for c in range(4)] + [ahead_force]
    behind_all = [behind_copy(c) for c in range(4)] + [behind_force]
    when(has_next, [copy.wait_send for copy in ahead_all] + [copy.wait_recv for copy in behind_all])
    when(has_prev, [copy.wait_recv for copy in ahead_all] + [copy.wait_send for copy in behind_all])

    def both(ref, at):
        return ref[(0, *at)] + ref[(1, *at)]

    more = both(got_force, (slice(0, 8), slice(0, 2 * TW)))
    blank = jnp.zeros((quarter, TW), f32)
    for g in range(4):
        extra = both(got, (g,))
        packed = jnp.concatenate(
            [extra[quarter : quarter + quarter // 2, 0:TW], extra[quarter : quarter + quarter // 2, TW:]], axis=0
        )
        for h in range(2):
            lanes = slice(h * TW, (h + 1) * TW)
            top = extra[0:quarter, lanes]
            turned = jnp.concatenate(
                [pltpu.roll(top, TW - quarter, 1), blank, pltpu.roll(top, quarter, 1), blank], axis=0
            ).T[0:quarter]
            corner = packed if h == 0 else pltpu.roll(packed, quarter, 1)
            total[g, 0:quarter, lanes] += top
            total[g, quarter:count, lanes] += jnp.where(upper, corner, turned)
            total[g, count : count + 8, lanes] += jnp.broadcast_to(more[g : g + 1, lanes], (8, TW))


def cycle(members, flow_east, flow_north, mixing, land, lists, counts, cells, values, noises, strips, groups):
    rows, width = members.shape[1:]
    slots = lists.shape[2]
    packed_rows = rows + rows // 4
    tiles = packed_rows // 2
    count = 8 * groups
    tables = [x.reshape(-1, TW) for x in (cells, values, noises)]
    big = [
        pltpu.with_memory_space_constraint(x, pltpu.HBM)
        for x in (members, flow_east, flow_north, mixing, land, lists, counts.reshape(1, rows))
    ]
    tables = [pltpu.with_memory_space_constraint(x, pltpu.HBM) for x in tables]
    dma = pltpu.SemaphoreType.DMA
    far_in = pl.BlockSpec(memory_space=pltpu.HBM)
    return pl.pallas_call(
        functools.partial(cycle_kernel, strips, groups),
        name="cycle",
        out_shape=[
            jax.ShapeDtypeStruct((tiles, count, 2 * TW), f32),
            jax.ShapeDtypeStruct((tiles, 2 * TW), f32),
            jax.ShapeDtypeStruct((4, count + 8, 4 * count), f32),
        ],
        in_specs=[far_in] * 10,
        out_specs=[pl.BlockSpec(memory_space=VMEM)] * 3,
        scratch_shapes=[
            VMEM(members.shape, f32),
            VMEM((rows, width), f32),
            VMEM((rows, width), f32),
            VMEM((rows, width), f32),
            VMEM((rows, width), i32),
            VMEM(lists.shape, i32),
            VMEM((1, rows), i32),
            VMEM(tables[0].shape, i32),
            VMEM(tables[1].shape, f32),
            VMEM(tables[2].shape, f32),
            VMEM((packed_rows, count, TW), f32),
            VMEM((rows + 2 * STEPS, 8, width), f32),
            VMEM((rows + 2 * STEPS, 8, width), f32),
            VMEM((rows + 2 * STEPS, 8, width), f32),
            VMEM((rows + 6, 4, width), f32),
            VMEM((groups, packed_rows, 8, TW), f32),
            VMEM((3 * rows, slots), i32),
            VMEM((3 * rows, slots), i32),
            VMEM((3 * rows, slots), i32),
            VMEM((3 * rows, slots), f32),
            VMEM((3 * rows, slots), f32),
            VMEM((3 * rows, tiles, 2 * TW), f32),
            VMEM((3 * rows, tiles, 2 * TW), f32),
            VMEM((tiles, 2 * TW, 2 * count), bf16),
            VMEM((4, 3 * count // 4, 4 * count), f32),
            VMEM((4, 3 * count // 4, 4 * count), f32),
            VMEM((2, 4, 3 * count // 4, 4 * count), f32),
            VMEM((8, 4 * count), f32),
            VMEM((8, 4 * count), f32),
            VMEM((2, 8, 4 * count), f32),
            dma((10,)), dma((6,)), dma((6,)), dma((2 * (groups - 1),)), dma((2 * (groups - 1),)), dma((2,)),
            dma((5,)), dma((5,)), dma((5,)), dma((5,)),
        ],
        compiler_params=pltpu.CompilerParams(
            collective_id=0, has_side_effects=True, vmem_limit_bytes=40 * 1024 * 1024
        ),
    )(*big, *tables)


def analysis_kernel(gram, centred, means, out, zs, rs, scales):
    quads, count, lanes = zs.shape
    per = lanes // count
    row_of = lax.broadcasted_iota(i32, (count, lanes), 0)
    lane_of = lax.broadcasted_iota(i32, (count, lanes), 1)
    eye = jnp.where(row_of == lane_of % count, 1.0, 0.0).astype(f32)
    seg_row = lax.broadcasted_iota(i32, (lanes, lanes), 0) // count
    seg_col = lax.broadcasted_iota(i32, (lanes, lanes), 1) // count
    diag = seg_row == seg_col
    diag_one = jnp.where(diag, 1.0, 0.0).astype(bf16)
    every = range(quads)

    def blocked(x):
        return jnp.where(diag, jnp.concatenate([x] * per, axis=0), jnp.zeros((), bf16))

    def right(x):
        return blocked(x[0]), blocked(x[1])

    def mul(a, b):
        (ah, al), (bh, bl) = a, b
        n = ah.shape[0]
        p = dot_nn(jnp.concatenate([ah, al], axis=0), bh)
        return p[:n] + p[n:] + dot_nn(ah, bl)

    b = [eye + gram[g, 0:count, :] / (count - 1) for g in every]
    stacked = []
    for g in every:
        sq = jnp.sum(b[g] * b[g], axis=0, keepdims=True)
        h1 = sq.astype(bf16)
        rest = sq - h1.astype(f32)
        h2 = rest.astype(bf16)
        h3 = (rest - h2.astype(f32)).astype(bf16)
        stacked += [jnp.broadcast_to(h, (16, lanes)) for h in (h1, h2, h3)]
    sums = dot_nn(jnp.concatenate(stacked, axis=0), diag_one)
    z, f = [], []
    for g in every:
        at = 48 * g
        frob = jnp.sqrt(sums[at : at + 1] + sums[at + 16 : at + 17] + sums[at + 32 : at + 33])
        z.append(b[g] / frob)
        scales[pl.ds(g, 1), :] = jnp.sqrt(frob)
        f.append(1.5 * eye - 0.5 * z[g])
        rs[g] = f[g]
    zr = [right(split(z[g])) for g in every]
    for g in every:
        zs[g] = mul(split(f[g]), zr[g])

    def step(i, _):
        r = [split(rs[g]) for g in every]
        z = [split(zs[g]) for g in every]
        zr = [right(z[g]) for g in every]
        f = [right(split(1.5 * eye - 0.5 * mul(r[g], zr[g]))) for g in every]
        for g in every:
            p = dot_nn(jnp.concatenate([z[g][0], z[g][1], r[g][0], r[g][1]], axis=0), f[g][0])
            q = dot_nn(jnp.concatenate([z[g][0], r[g][0]], axis=0), f[g][1])
            zs[g] = p[:count] + p[count : 2 * count] + q[:count]
            rs[g] = p[2 * count : 3 * count] + p[3 * count :] + q[count:]
        return 0

    lax.fori_loop(0, NSITER - 2, step, 0, unroll=3)
    low_half = lax.broadcasted_iota(i32, (count, 2 * count), 1) < count
    r = [split(rs[g]) for g in every]
    zr = [right(split(zs[g])) for g in every]
    f = [right(split(1.5 * eye - 0.5 * mul(r[g], zr[g]))) for g in every]
    t = [mul(r[g], f[g]) / scales[pl.ds(g, 1), :] for g in every]
    tr = [right(split(t[g])) for g in every]
    vec = [jnp.broadcast_to(gram[g, count : count + 1, :], (16, lanes)) for g in every]
    vec = [mul(split(vec[g]), tr[g]) for g in every]
    vec = [mul(split(vec[g]), tr[g]) / (count - 1) for g in every]
    for g in every:
        mix = t[g] + vec[g][0:1]
        for h in range(per // 2):
            two = mix[:, h * 2 * count : (h + 1) * 2 * count]
            pair = g * (per // 2) + h
            k = PAIR_AT[pair]
            x = split(jnp.concatenate([centred[k, :, 0:TW], centred[k, :, TW : 2 * TW]], axis=0))
            lhs = jnp.concatenate([jnp.where(low_half, two, 0.0), jnp.where(low_half, 0.0, two)], axis=0)
            y = mul(split(lhs), x)
            for q in range(2):
                average = means[k : k + 1, q * TW : (q + 1) * TW]
                out[:, 2 * pair + q, :] = average + y[q * count : (q + 1) * count]


def analyse(gram, centred, means, rows):
    quads, _, lanes = gram.shape
    count = centred.shape[1]
    return pl.pallas_call(
        analysis_kernel,
        name="analysis",
        out_shape=jax.ShapeDtypeStruct((count, rows, TW), f32),
        in_specs=[pl.BlockSpec(memory_space=VMEM)] * 3,
        out_specs=pl.BlockSpec(memory_space=VMEM),
        scratch_shapes=[
            VMEM((quads, count, lanes), f32),
            VMEM((quads, count, lanes), f32),
            VMEM((quads, lanes), f32),
        ],
        compiler_params=pltpu.CompilerParams(vmem_limit_bytes=16 * 1024 * 1024),
    )(gram, centred, means)


def body(strips, groups, members, flow_east, flow_north, mixing, land_mask, sensor_cell,
         sensor_value, sensor_noise, tile_lists, tile_counts):
    centred, means, total = cycle(
        members, flow_east, flow_north, mixing, land_mask, tile_lists, tile_counts,
        sensor_cell, sensor_value, sensor_noise, strips, groups,
    )
    return analyse(total, centred, means, members.shape[1])


def solution(mesh):
    strips, groups = mesh.shape["space"], mesh.shape["mem"]
    in_specs = (
        P("mem", "space", None),
        P("space", None),
        P("space", None),
        P("space", None),
        P("space", None),
        P("space"),
        P("space"),
        P("space"),
        P("space", "mem", None),
        P("space", "mem"),
    )
    return jax.shard_map(
        functools.partial(body, strips, groups),
        mesh=mesh,
        in_specs=in_specs,
        out_specs=P(None, "space", "mem"),
        check_vma=False,
    )
```
